32 devices in a mesh: dp: 1 (over z), tp: 4 (over y), ep: 8 (over x, core).
Axes of the slice: x: 4, y: 4, z: 1, core: 2. Of those that a mesh axis runs over, the one named last changes fastest.
The devices are a block of a 4x4x8 slice.
Arguments:
- hidden: bfloat16 [2048, 768], P(('dp', 'ep'))
- write_pos: int32 [2048], P(('dp', 'ep'))
- enc_mask: int32 [2048, 32], P(('dp', 'ep'))
- expert_idx: int32 [2048], P(('dp', 'ep'))
- self_keys: bfloat16 [2, 2048, 12, 32, 64], P(None, ('dp', 'ep'), 'tp')
- self_values: bfloat16 [2, 2048, 12, 32, 64], P(None, ('dp', 'ep'), 'tp')
- cross_keys: bfloat16 [2, 2048, 12, 32, 64], P(None, ('dp', 'ep'), 'tp')
- cross_values: bfloat16 [2, 2048, 12, 32, 64], P(None, ('dp', 'ep'), 'tp')
- rel_bias: float32 [12, 32], P('tp')
- norm_scale: float32 [2, 3, 768], replicated
- w_query: bfloat16 [2, 768, 768], P(None, None, 'tp')
- w_key: bfloat16 [2, 768, 768], P(None, None, 'tp')
- w_value: bfloat16 [2, 768, 768], P(None, None, 'tp')
- w_out: bfloat16 [2, 768, 768], P(None, 'tp')
- w_cross_query: bfloat16 [2, 768, 768], P(None, None, 'tp')
- w_cross_out: bfloat16 [2, 768, 768], P(None, 'tp')
- dense_gate: bfloat16 [768, 3072], P(None, 'tp')
- dense_up: bfloat16 [768, 3072], P(None, 'tp')
- dense_down: bfloat16 [3072, 768], P('tp')
- router: float32 [768, 16], replicated
- exp_gate: bfloat16 [16, 768, 3072], P('ep', None, 'tp')
- exp_up: bfloat16 [16, 768, 3072], P('ep', None, 'tp')
- exp_down: bfloat16 [16, 3072, 768], P('ep', 'tp')
Outputs:
- output 1: bfloat16 [2048, 768], P(('dp', 'ep'))
- output 2: bfloat16 [2, 2048, 12, 32, 64], P(None, ('dp', 'ep'), 'tp')
- output 3: bfloat16 [2, 2048, 12, 32, 64], P(None, ('dp', 'ep'), 'tp')
All inputs are finite; a program needn't handle non-finite values.
Results may differ from the reference program's by a relative error of at most 0.02.
Values are sent between devices in bfloat16 or wider.
A program may use at most 768 MiB of HBM per device.

```python
import jax
import jax.numpy as jnp
from jax import lax

D = 768
HEADS = 12
HEAD = 64
FF = 3072
EXPERTS = 16
TOK_DEV = 256
GROUPS = 8
CACHE = 32
SRC = 32
TOKENS = TOK_DEV * GROUPS
WIDTH = HEADS * HEAD
CAPACITY = (2 * TOK_DEV + EXPERTS - 1) // EXPERTS
EPS = 1e-6
NEG_BIG = -1e9


def setup_inputs(seed: int = 0, part: int = 0) -> dict:
    root = jax.random.key(seed)
    shared_root, part_root = jax.random.split(root)
    local = jax.random.fold_in(part_root, part)
    local_keys = jax.random.split(local, 10)
    shared_keys = jax.random.split(shared_root, 16)

    def normal(key, shape, scale):
        return jax.random.normal(key, shape, jnp.float32) * scale

    row_ids = jnp.arange(TOKENS)
    hidden = normal(local_keys[0], (TOKENS, D), 1.0).astype(jnp.bfloat16)
    pos_draw = jax.random.randint(local_keys[1], (TOKENS,), 0, CACHE)
    write_pos = jnp.where(row_ids == 0, CACHE - 1, pos_draw).astype(jnp.int32)
    src_len = jax.random.randint(local_keys[2], (TOKENS,), max(SRC // 4, 1), SRC + 1)
    src_len = jnp.where(row_ids == 1, SRC, src_len)
    enc_mask = (jnp.arange(SRC)[None, :] < src_len[:, None]).astype(jnp.int32)
    spread = jax.random.permutation(local_keys[3], TOKENS) % EXPERTS
    hot_expert = jax.random.randint(local_keys[4], (), 0, EXPERTS)
    to_hot = jax.random.randint(local_keys[5], (TOKENS,), 0, 4) == 0
    expert_idx = jnp.where(to_hot, hot_expert, spread).astype(jnp.int32)
    self_shape = (2, TOKENS, HEADS, CACHE, HEAD)
    cross_shape = (2, TOKENS, HEADS, SRC, HEAD)
    return {
        'hidden': hidden,
        'write_pos': write_pos,
        'enc_mask': enc_mask,
        'expert_idx': expert_idx,
        'self_keys': normal(local_keys[6], self_shape, 1.0).astype(jnp.bfloat16),
        'self_values': normal(local_keys[7], self_shape, 1.0).astype(jnp.bfloat16),
        'cross_keys': normal(local_keys[8], cross_shape, 1.0).astype(jnp.bfloat16),
        'cross_values': normal(local_keys[9], cross_shape, 1.0).astype(jnp.bfloat16),
        'rel_bias': normal(shared_keys[0], (HEADS, CACHE), 1.0),
        'norm_scale': jax.random.uniform(shared_keys[1], (2, 3, D), jnp.float32, 0.5, 1.5),
        'w_query': normal(shared_keys[2], (2, D, WIDTH), 2.0 * (D * HEAD) ** -0.5).astype(jnp.bfloat16),
        'w_key': normal(shared_keys[3], (2, D, WIDTH), D ** -0.5).astype(jnp.bfloat16),
        'w_value': normal(shared_keys[4], (2, D, WIDTH), D ** -0.5).astype(jnp.bfloat16),
        'w_out': normal(shared_keys[5], (2, WIDTH, D), WIDTH ** -0.5).astype(jnp.bfloat16),
        'w_cross_query': normal(shared_keys[6], (2, D, WIDTH), 2.0 * (D * HEAD) ** -0.5).astype(jnp.bfloat16),
        'w_cross_out': normal(shared_keys[7], (2, WIDTH, D), WIDTH ** -0.5).astype(jnp.bfloat16),
        'dense_gate': normal(shared_keys[8], (D, FF), D ** -0.5).astype(jnp.bfloat16),
        'dense_up': normal(shared_keys[9], (D, FF), D ** -0.5).astype(jnp.bfloat16),
        'dense_down': normal(shared_keys[10], (FF, D), FF ** -0.5).astype(jnp.bfloat16),
        'router': normal(shared_keys[11], (D, EXPERTS), 2.0 * D ** -0.5),
        'exp_gate': normal(shared_keys[12], (EXPERTS, D, FF), D ** -0.5).astype(jnp.bfloat16),
        'exp_up': normal(shared_keys[13], (EXPERTS, D, FF), D ** -0.5).astype(jnp.bfloat16),
        'exp_down': normal(shared_keys[14], (EXPERTS, FF, D), 0.5 * (EXPERTS / FF) ** 0.5).astype(jnp.bfloat16),
    }


def rms_norm(h_cur, scale):
    h_float = h_cur.astype(jnp.float32)
    inv_rms = lax.rsqrt(jnp.mean(h_float * h_float, axis=-1, keepdims=True) + EPS)
    return (h_float * inv_rms * scale).astype(jnp.bfloat16)


def add_residual(h_cur, delta):
    return (h_cur.astype(jnp.float32) + delta.astype(jnp.float32)).astype(jnp.bfloat16)


def project(normed, weight):
    return jnp.dot(normed, weight, preferred_element_type=jnp.float32)


def self_attention(normed, write_pos, keys, values, w_query, w_key, w_value, w_out, rel_bias):
    tokens = normed.shape[0]
    query = project(normed, w_query).astype(jnp.bfloat16).reshape(tokens, HEADS, HEAD)
    key_new = project(normed, w_key).astype(jnp.bfloat16).reshape(tokens, HEADS, HEAD)
    value_new = project(normed, w_value).astype(jnp.bfloat16).reshape(tokens, HEADS, HEAD)
    distance = write_pos[:, None] - jnp.arange(CACHE)[None, :]
    at_slot = (distance == 0)[:, None, :, None]
    keys = jnp.where(at_slot, key_new[:, :, None, :], keys)
    values = jnp.where(at_slot, value_new[:, :, None, :], values)
    scores = jnp.einsum('thd,thld->thl', query.astype(jnp.float32), keys.astype(jnp.float32))
    bias = jnp.take(rel_bias, jnp.maximum(distance, 0), axis=1)
    scores = jnp.where((distance >= 0)[:, None, :], scores + jnp.swapaxes(bias, 0, 1), NEG_BIG)
    attn_prob = jax.nn.softmax(scores, axis=-1).astype(jnp.bfloat16)
    context = jnp.einsum('thl,thld->thd', attn_prob.astype(jnp.float32), values.astype(jnp.float32)).astype(jnp.bfloat16)
    attn_out = project(context.reshape(tokens, WIDTH), w_out).astype(jnp.bfloat16)
    return attn_out, keys, values


def cross_attention(normed, enc_mask, keys, values, w_query, w_out):
    tokens = normed.shape[0]
    query = project(normed, w_query).astype(jnp.bfloat16).reshape(tokens, HEADS, HEAD)
    scores = jnp.einsum('thd,thsd->ths', query.astype(jnp.float32), keys.astype(jnp.float32))
    scores = jnp.where((enc_mask > 0)[:, None, :], scores, NEG_BIG)
    attn_prob = jax.nn.softmax(scores, axis=-1).astype(jnp.bfloat16)
    context = jnp.einsum('ths,thsd->thd', attn_prob.astype(jnp.float32), values.astype(jnp.float32)).astype(jnp.bfloat16)
    return project(context.reshape(tokens, WIDTH), w_out).astype(jnp.bfloat16)


def gated_ffn(normed, w_gate, w_up, w_down):
    product = (jax.nn.gelu(project(normed, w_gate)) * project(normed, w_up)).astype(jnp.bfloat16)
    return project(product, w_down).astype(jnp.bfloat16)


def switch_ffn(normed, expert_idx, router, exp_gate, exp_up, exp_down):
    logits = jnp.dot(normed.astype(jnp.float32), router)
    route_prob = jax.nn.softmax(logits, axis=-1)
    gate = jnp.take_along_axis(route_prob, expert_idx[:, None], axis=1)[:, 0]
    onehot = (expert_idx[:, None] == jnp.arange(EXPERTS)[None, :]).astype(jnp.int32)
    onehot = onehot.reshape(GROUPS, TOK_DEV, EXPERTS)
    slot = jnp.sum((jnp.cumsum(onehot, axis=1) - onehot) * onehot, axis=2)
    dispatch = (onehot[..., None] * (slot[:, :, None, None] == jnp.arange(CAPACITY))).astype(jnp.float32)
    x_groups = normed.reshape(GROUPS, TOK_DEV, D).astype(jnp.float32)
    buffers = jnp.einsum('gtec,gtd->egcd', dispatch, x_groups).astype(jnp.bfloat16)
    buffers = buffers.reshape(EXPERTS, GROUPS * CAPACITY, D)

    def run_expert(expert):
        rows, w_gate, w_up, w_down = expert
        return gated_ffn(rows, w_gate, w_up, w_down)

    expert_out = lax.map(run_expert, (buffers, exp_gate, exp_up, exp_down))
    expert_out = expert_out.reshape(EXPERTS, GROUPS, CAPACITY, D).astype(jnp.float32)
    combined = jnp.einsum('gtec,egcd->gtd', dispatch, expert_out).reshape(TOKENS, D)
    return gate[:, None] * combined


def attention_block(layer, h_cur, write_pos, enc_mask, self_keys, self_values, cross_keys, cross_values, rel_bias, norm_scale, w_query, w_key, w_value, w_out, w_cross_query, w_cross_out):
    def one_group(group):
        h_grp, pos_grp, mask_grp, keys_grp, values_grp, ckeys_grp, cvalues_grp = group
        normed = rms_norm(h_grp, norm_scale[layer, 0])
        attn_out, keys_grp, values_grp = self_attention(normed, pos_grp, keys_grp, values_grp, w_query[layer], w_key[layer], w_value[layer], w_out[layer], rel_bias)
        h_grp = add_residual(h_grp, attn_out)
        normed = rms_norm(h_grp, norm_scale[layer, 1])
        cross_out = cross_attention(normed, mask_grp, ckeys_grp, cvalues_grp, w_cross_query[layer], w_cross_out[layer])
        return add_residual(h_grp, cross_out), keys_grp, values_grp

    def grouped(array_in):
        return array_in.reshape((GROUPS, TOK_DEV) + array_in.shape[1:])

    h_grp, keys_new, values_new = lax.map(one_group, (grouped(h_cur), grouped(write_pos), grouped(enc_mask), grouped(self_keys[layer]), grouped(self_values[layer]), grouped(cross_keys[layer]), grouped(cross_values[layer])))
    return h_grp.reshape(TOKENS, D), keys_new.reshape(self_keys.shape[1:]), values_new.reshape(self_values.shape[1:])


def reference(hidden, write_pos, enc_mask, expert_idx, self_keys, self_values, cross_keys, cross_values, rel_bias, norm_scale, w_query, w_key, w_value, w_out, w_cross_query, w_cross_out, dense_gate, dense_up, dense_down, router, exp_gate, exp_up, exp_down):
    h_cur, keys_a, values_a = attention_block(0, hidden, write_pos, enc_mask, self_keys, self_values, cross_keys, cross_values, rel_bias, norm_scale, w_query, w_key, w_value, w_out, w_cross_query, w_cross_out)
    normed = rms_norm(h_cur, norm_scale[0, 2])
    h_cur = add_residual(h_cur, gated_ffn(normed, dense_gate, dense_up, dense_down))
    h_cur, keys_b, values_b = attention_block(1, h_cur, write_pos, enc_mask, self_keys, self_values, cross_keys, cross_values, rel_bias, norm_scale, w_query, w_key, w_value, w_out, w_cross_query, w_cross_out)
    normed = rms_norm(h_cur, norm_scale[1, 2])
    h_cur = add_residual(h_cur, switch_ffn(normed, expert_idx, router, exp_gate, exp_up, exp_down))
    return h_cur, jnp.stack([keys_a, keys_b]), jnp.stack([values_a, values_b])
```

```python
import functools

import jax
import jax.numpy as jnp
from jax import lax
from jax.experimental import pallas as pl
from jax.experimental.pallas import tpu as pltpu
from jax.sharding import PartitionSpec as P

EPS = 1e-6
NEG_BIG = -1e9
MESH = pl.DeviceIdType.MESH
LANES = 128
VMEM = pl.BlockSpec(memory_space=pltpu.VMEM)
ANY = pl.BlockSpec(memory_space=pl.ANY)
VMEM_LIMIT = 60 * 1024 * 1024

NT = (((1,), (1,)), ((), ()))
NN = (((1,), (0,)), ((), ()))
TN = (((0,), (0,)), ((), ()))


def dot(a, b, dims=NN, **kw):
    return lax.dot_general(a, b, dims, preferred_element_type=jnp.float32, **kw)


def rms_norm(h, scale):
    h = h.astype(jnp.float32)
    inv = lax.rsqrt(jnp.mean(h * h, axis=-1, keepdims=True) + EPS)
    return (h * inv * scale).astype(jnp.bfloat16)


def softmax_rows(s):
    p = jnp.exp(s - jnp.max(s, axis=0, keepdims=True))
    return (p / jnp.sum(p, axis=0, keepdims=True)).astype(jnp.bfloat16).astype(jnp.float32)


def slot_scores(query, load, slots):
    rows = [jnp.sum(load(j).astype(jnp.float32) * query, axis=0, keepdims=True) for j in range(slots)]
    return jnp.concatenate(rows, axis=0)


def self_kernel(layer, h_ref, scale_ref, pos_ref, bias_ref, wq_ref, wk_ref, wv_ref, k_ref, v_ref, *rest):
    ctx_ref, ko_ref, vo_ref, q_s, k_s, v_s, b_s = rest[-7:]
    heads, halves, dim, lanes = q_s.shape
    slots = k_ref.shape[2]
    step = pl.program_id(0)

    @pl.when(step == 0)
    def _():
        x = rms_norm(h_ref[...], scale_ref[...])
        qt = dot(wq_ref[...], x, NT).astype(jnp.bfloat16)
        kt = dot(wk_ref[...], x, NT).astype(jnp.bfloat16)
        vt = dot(wv_ref[...], x, NT).astype(jnp.bfloat16)
        tokens = x.shape[0]
        onehot = (lax.broadcasted_iota(jnp.int32, (LANES, tokens), 0) == pos_ref[...]).astype(jnp.float32)
        for a in range(heads):
            row = jnp.concatenate([bias_ref[a:a + 1, :], jnp.zeros((1, LANES - slots), jnp.float32)], axis=1)
            table = pltpu.roll(jnp.broadcast_to(row, (slots, LANES)), 0, 1, stride=1, stride_axis=0)
            bias = dot(table, onehot, precision=lax.Precision.HIGHEST)
            for b in range(halves):
                rs, cs = slice(a * dim, (a + 1) * dim), slice(b * lanes, (b + 1) * lanes)
                q_s[a, b] = qt[rs, cs].astype(jnp.float32)
                k_s[a, b] = kt[rs, cs]
                v_s[a, b] = vt[rs, cs]
                b_s[a, b] = bias[:, cs]

    head, half = step // halves, step % halves
    pos = pos_ref[:, pl.ds(pl.multiple_of(half * lanes, lanes), lanes)]
    pos_bf = jnp.broadcast_to(pos.astype(jnp.float32), (dim, lanes)).astype(jnp.bfloat16)
    query, k_new, v_new = q_s[head, half], k_s[head, half], v_s[head, half]
    slot_id = lax.broadcasted_iota(jnp.int32, (slots, lanes), 0)

    rows = []
    for j in range(slots):
        old = k_ref[0, 0, j]
        ko_ref[0, 0, j] = jnp.where(pos_bf == jnp.bfloat16(j), k_new, old)
        rows.append(jnp.sum(old.astype(jnp.float32) * query, axis=0, keepdims=True))
    scores = jnp.concatenate(rows, axis=0)
    new_score = jnp.sum(k_new.astype(jnp.float32) * query, axis=0, keepdims=True)
    at_slot = slot_id == pos
    scores = jnp.where(at_slot, new_score, scores)
    scores = jnp.where(slot_id <= pos, scores + b_s[head, half], NEG_BIG)
    prob = softmax_rows(scores)
    prob_new = jnp.sum(jnp.where(at_slot, prob, 0.0), axis=0, keepdims=True)
    prob_old = jnp.where(at_slot, 0.0, prob)
    acc = v_new.astype(jnp.float32) * prob_new
    for j in range(slots):
        old = v_ref[0, 0, j]
        vo_ref[0, 0, j] = jnp.where(pos_bf == jnp.bfloat16(j), v_new, old)
        acc += old.astype(jnp.float32) * prob_old[j:j + 1, :]
    ctx_ref[...] = acc.astype(jnp.bfloat16)


def self_attention(layer, h, scale, pos, rel_bias, wq, wk, wv, keys, values, prev):
    tokens, width = h.shape
    _, heads, slots, dim, _ = keys.shape
    halves = tokens // LANES
    cache = pl.BlockSpec((1, 1, slots, dim, LANES), lambda i: (layer, i // halves, 0, 0, i % halves))
    full = lambda a: pl.BlockSpec(a.shape, lambda i: (0,) * a.ndim)
    args = [h, scale, pos, rel_bias, wq, wk, wv, keys, values]
    specs = [full(a) for a in args[:7]] + [cache, cache]
    aliases = {}
    if prev is not None:
        aliases = {len(args): 1, len(args) + 1: 2}
        args += list(prev)
        specs += [ANY, ANY]
    return pl.pallas_call(
        functools.partial(self_kernel, layer),
        grid=(heads * halves,),
        out_shape=(jax.ShapeDtypeStruct((heads * dim, tokens), jnp.bfloat16), jax.ShapeDtypeStruct(keys.shape, keys.dtype), jax.ShapeDtypeStruct(values.shape, values.dtype)),
        in_specs=specs,
        out_specs=(pl.BlockSpec((dim, LANES), lambda i: (i // halves, i % halves)), cache, cache),
        scratch_shapes=[
            pltpu.VMEM((heads, halves, dim, LANES), jnp.float32),
            pltpu.VMEM((heads, halves, dim, LANES), jnp.bfloat16),
            pltpu.VMEM((heads, halves, dim, LANES), jnp.bfloat16),
            pltpu.VMEM((heads, halves, slots, LANES), jnp.float32),
        ],
        input_output_aliases=aliases,
        compiler_params=pltpu.CompilerParams(vmem_limit_bytes=VMEM_LIMIT, dimension_semantics=("arbitrary",)),
        name=f"self_attention_{layer}",
    )(*args)


def cross_attention(x, mask_ref, wq, k_buf, v_buf, ctx_s, q_s):
    heads, slots, dim, tokens = k_buf.shape
    halves = tokens // LANES
    qt = dot(wq, x, NT).astype(jnp.bfloat16)
    for a in range(heads):
        q_s[a] = qt[a * dim:(a + 1) * dim, :].astype(jnp.float32)

    def one_head(a, carry):
        for b in range(halves):
            cs = slice(b * LANES, (b + 1) * LANES)
            scores = slot_scores(q_s[a, :, cs], lambda j: k_buf[a, j, :, cs], slots)
            prob = softmax_rows(jnp.where(mask_ref[:, cs] > 0, scores, NEG_BIG))
            acc = jnp.zeros((dim, LANES), jnp.float32)
            for j in range(slots):
                acc += v_buf[a, j, :, cs].astype(jnp.float32) * prob[j:j + 1, :]
            ctx_s[a, :, cs] = acc.astype(jnp.bfloat16)
        return carry

    lax.fori_loop(0, heads, one_head, 0)
    return ctx_s[...].reshape(heads * dim, tokens)


def enter(peers):
    barrier = pltpu.get_barrier_semaphore()
    for axis, index in peers:
        pl.semaphore_signal(barrier, inc=1, device_id={axis: index}, device_id_type=MESH)
    pl.semaphore_wait(barrier, len(peers))


class Group:
    def __init__(self, axis, n, sems):
        self.axis, self.n, self.me = axis, n, lax.axis_index(axis)
        self.send, self.recv = sems

    def peer(self, k):
        return lax.rem(self.me + k, self.n)

    def peers(self):
        return [(self.axis, self.peer(k)) for k in range(1, self.n)]

    def exchange(self, phase, src, dst):
        copies = []
        for k in range(1, self.n):
            copy = pltpu.make_async_remote_copy(
                src_ref=src(k, self.peer(k)),
                dst_ref=dst(k, self.peer(k)),
                send_sem=self.send.at[phase, k - 1],
                recv_sem=self.recv.at[phase, k - 1],
                device_id={self.axis: self.peer(k)},
                device_id_type=MESH,
            )
            copy.start()
            copies.append(copy)
        return copies


def sum_over_tp(tp, phase, part, part_s, in_s, h_ref, out_s, gate_ref=None):
    tokens = part.shape[0]
    rows = tokens // tp.n
    part_s[...] = part.astype(jnp.bfloat16)
    block = lambda i: pl.ds(pl.multiple_of(i * rows, rows), rows)
    copies = tp.exchange(2 * phase, lambda k, i: part_s.at[block(i)], lambda k, i: in_s.at[phase, k - 1])
    total = part_s[block(tp.me), :].astype(jnp.float32)
    for k, copy in enumerate(copies):
        copy.wait_recv()
        total += in_s[phase, k].astype(jnp.float32)
    total = total.astype(jnp.bfloat16).astype(jnp.float32)
    if gate_ref is not None:
        total = total * gate_ref[block(tp.me), :]
    out_s[block(tp.me), :] = (h_ref[block(tp.me), :].astype(jnp.float32) + total).astype(jnp.bfloat16)
    mine = out_s.at[block(tp.me)]
    spread = tp.exchange(2 * phase + 1, lambda k, i: mine, lambda k, i: mine)
    for copy in spread:
        copy.wait_recv()
    return copies + spread


def gelu_product(gate, up):
    return (jax.nn.gelu(gate) * up).astype(jnp.bfloat16)


def loader(sems):
    pending = {}

    def start(name, src, dst):
        copy = pltpu.make_async_copy(src, dst, sems.at[len(pending)])
        copy.start()
        pending[name] = copy

    return start, pending


def dense_kernel(n_tp, layer, h_ref, ctx_ref, scale_ref, mask_ref, wo_ref, wcq_ref, wco_ref, wg_ref, wu_ref, wd_ref, ck_ref, cv_ref, out_ref,
                 k_buf, v_buf, wo, wcq, wco, wg, wu, wd, q_s, ctx_s, part_s, in_s, h1, h2, load_sem, tp_send, tp_recv):
    start, pending = loader(load_sem)
    start("wo", wo_ref.at[layer], wo)
    start("wcq", wcq_ref.at[layer], wcq)
    start("ck", ck_ref.at[layer], k_buf)
    start("cv", cv_ref.at[layer], v_buf)
    start("wco", wco_ref.at[layer], wco)
    start("wg", wg_ref, wg)
    start("wu", wu_ref, wu)
    start("wd", wd_ref, wd)
    tp = Group("tp", n_tp, (tp_send, tp_recv))
    enter(tp.peers())

    pending["wo"].wait()
    sent = sum_over_tp(tp, 0, dot(ctx_ref[...], wo[...], TN), part_s.at[0], in_s, h_ref, h1)
    x = rms_norm(h1[...], scale_ref[1:2, :])
    for name in ("wcq", "ck", "cv", "wco"):
        pending[name].wait()
    ctx = cross_attention(x, mask_ref, wcq[...], k_buf, v_buf, ctx_s, q_s)
    sent += sum_over_tp(tp, 1, dot(ctx, wco[...], TN), part_s.at[1], in_s, h1, h2)
    x = rms_norm(h2[...], scale_ref[2:3, :])
    for name in ("wg", "wu", "wd"):
        pending[name].wait()
    product = gelu_product(dot(x, wg[...]), dot(x, wu[...]))
    sent += sum_over_tp(tp, 2, dot(product, wd[...]), part_s.at[2], in_s, h2, out_ref)
    for copy in sent:
        copy.wait_send()


def dense_block(n_tp, layer, h, ctx, scale, mask, w_out, w_cq, w_co, w_gate, w_up, w_down, cross_k, cross_v):
    tokens, width = h.shape
    _, heads, slots, dim, _ = cross_k.shape
    rows = tokens // n_tp
    bf = lambda *s: pltpu.VMEM(s, jnp.bfloat16)
    return pl.pallas_call(
        functools.partial(dense_kernel, n_tp, layer),
        out_shape=jax.ShapeDtypeStruct(h.shape, h.dtype),
        in_specs=[VMEM] * 4 + [ANY] * 8,
        out_specs=VMEM,
        scratch_shapes=[
            bf(*cross_k.shape[1:]), bf(*cross_v.shape[1:]), bf(*w_out.shape[1:]), bf(*w_cq.shape[1:]), bf(*w_co.shape[1:]),
            bf(*w_gate.shape), bf(*w_up.shape), bf(*w_down.shape),
            pltpu.VMEM((heads, dim, tokens), jnp.float32), bf(heads, dim, tokens),
            bf(3, tokens, width), bf(3, n_tp - 1, rows, width), bf(tokens, width), bf(tokens, width),
            pltpu.SemaphoreType.DMA((8,)), pltpu.SemaphoreType.DMA((6, n_tp - 1)), pltpu.SemaphoreType.DMA((6, n_tp - 1)),
        ],
        compiler_params=pltpu.CompilerParams(vmem_limit_bytes=VMEM_LIMIT, collective_id=0, has_side_effects=True),
        name="block_a",
    )(h, ctx, scale, mask, w_out, w_cq, w_co, w_gate, w_up, w_down, cross_k, cross_v)


def routing(idx_row, idx_col, experts):
    tokens = idx_row.shape[1]
    capacity = (2 * tokens + experts - 1) // experts
    one_t = lax.broadcasted_iota(jnp.int32, (experts, tokens), 0) == idx_row
    one = lax.broadcasted_iota(jnp.int32, (tokens, experts), 1) == idx_col
    earlier = lax.broadcasted_iota(jnp.int32, (tokens, tokens), 0) < lax.broadcasted_iota(jnp.int32, (tokens, tokens), 1)
    later = lax.broadcasted_iota(jnp.int32, (tokens, tokens), 0) > lax.broadcasted_iota(jnp.int32, (tokens, tokens), 1)
    to_bf = lambda m: m.astype(jnp.float32).astype(jnp.bfloat16)
    count_t = dot(to_bf(one_t), to_bf(earlier))
    count = dot(to_bf(later), to_bf(one))
    slot_row = jnp.sum(jnp.where(one_t, count_t, 0.0), axis=0, keepdims=True)
    slot_col = jnp.sum(jnp.where(one, count, 0.0), axis=1, keepdims=True)
    place = lambda slot, idx: jnp.where(slot < capacity, idx.astype(jnp.float32) * capacity + slot, -1.0)
    return place(slot_row, idx_row), place(slot_col, idx_col), one, capacity


def moe_kernel(n_tp, n_ep, layer, h_ref, ctx_ref, scale_ref, mask_ref, idx_row_ref, idx_col_ref, router_ref, wo_ref, wcq_ref, wco_ref, wg_ref, wu_ref, wd_ref, ck_ref, cv_ref, out_ref,
               k_buf, v_buf, wo, wcq, wco, wg, wu, wd, q_s, ctx_s, part_s, in_s, h1, h2, disp, x_in, y_out, y_in, gate_s, load_sem, tp_send, tp_recv, ep_send, ep_recv):
    start, pending = loader(load_sem)
    start("wo", wo_ref.at[layer], wo)
    start("wcq", wcq_ref.at[layer], wcq)
    start("ck", ck_ref.at[layer], k_buf)
    start("cv", cv_ref.at[layer], v_buf)
    start("wco", wco_ref.at[layer], wco)
    start("wg", wg_ref, wg)
    start("wu", wu_ref, wu)
    start("wd", wd_ref, wd)
    tp = Group("tp", n_tp, (tp_send, tp_recv))
    ep = Group("ep", n_ep, (ep_send, ep_recv))
    enter(tp.peers() + ep.peers())

    pending["wo"].wait()
    sent = sum_over_tp(tp, 0, dot(ctx_ref[...], wo[...], TN), part_s.at[0], in_s, h_ref, h1)
    x = rms_norm(h1[...], scale_ref[1:2, :])
    for name in ("wcq", "ck", "cv", "wco"):
        pending[name].wait()
    ctx = cross_attention(x, mask_ref, wcq[...], k_buf, v_buf, ctx_s, q_s)
    sent += sum_over_tp(tp, 1, dot(ctx, wco[...], TN), part_s.at[1], in_s, h1, h2)

    x = rms_norm(h2[...], scale_ref[2:3, :])
    tokens, width = x.shape
    experts = router_ref.shape[0]
    local = experts // n_ep
    place_row, place_col, one, capacity = routing(idx_row_ref[...], idx_col_ref[...], experts)
    spots = experts * capacity
    to_bf = lambda m: m.astype(jnp.float32).astype(jnp.bfloat16)
    pick = to_bf(lax.broadcasted_iota(jnp.int32, (spots, tokens), 0).astype(jnp.float32) == place_row)
    disp[...] = dot(pick, x).astype(jnp.bfloat16).reshape(disp.shape)
    x_in[ep.me] = disp[ep.me]
    there = ep.exchange(0, lambda k, i: disp.at[i], lambda k, i: x_in.at[ep.me])
    logits = dot(x.astype(jnp.float32), router_ref[...], NT, precision=lax.Precision.HIGHEST)
    prob = jnp.exp(logits - jnp.max(logits, axis=1, keepdims=True))
    prob = prob / jnp.sum(prob, axis=1, keepdims=True)
    gate_s[...] = jnp.sum(jnp.where(one, prob, 0.0), axis=1, keepdims=True)
    for name in ("wg", "wu", "wd"):
        pending[name].wait()
    for copy in there:
        copy.wait_recv()
    for j in range(local):
        rows = x_in[:, j].reshape(n_ep * capacity, width)
        product = gelu_product(dot(rows, wg[j]), dot(rows, wu[j]))
        y_out[:, j] = dot(product, wd[j]).astype(jnp.bfloat16).reshape(n_ep, capacity, width)
    y_in[ep.me] = y_out[ep.me]
    back = ep.exchange(1, lambda k, i: y_out.at[i], lambda k, i: y_in.at[ep.me])
    put = to_bf(lax.broadcasted_iota(jnp.int32, (tokens, spots), 1).astype(jnp.float32) == place_col)
    for copy in back:
        copy.wait_recv()
    part = dot(put, y_in[...].reshape(spots, width))
    sent += sum_over_tp(tp, 2, part, part_s.at[2], in_s, h2, out_ref, gate_s)
    for copy in sent + there + back:
        copy.wait_send()


def moe_block(n_tp, n_ep, layer, h, ctx, scale, mask, idx_row, idx_col, router, w_out, w_cq, w_co, w_gate, w_up, w_down, cross_k, cross_v):
    tokens, width = h.shape
    _, heads, slots, dim, _ = cross_k.shape
    rows = tokens // n_tp
    experts = router.shape[0]
    capacity = (2 * tokens + experts - 1) // experts
    bf = lambda *s: pltpu.VMEM(s, jnp.bfloat16)
    spots = (n_ep, experts // n_ep, capacity, width)
    return pl.pallas_call(
        functools.partial(moe_kernel, n_tp, n_ep, layer),
        out_shape=jax.ShapeDtypeStruct(h.shape, h.dtype),
        in_specs=[VMEM] * 7 + [ANY] * 8,
        out_specs=VMEM,
        scratch_shapes=[
            bf(*cross_k.shape[1:]), bf(*cross_v.shape[1:]), bf(*w_out.shape[1:]), bf(*w_cq.shape[1:]), bf(*w_co.shape[1:]),
            bf(*w_gate.shape), bf(*w_up.shape), bf(*w_down.shape),
            pltpu.VMEM((heads, dim, tokens), jnp.float32), bf(heads, dim, tokens),
            bf(3, tokens, width), bf(3, n_tp - 1, rows, width), bf(tokens, width), bf(tokens, width),
            bf(*spots), bf(*spots), bf(*spots), bf(*spots), pltpu.VMEM((tokens, 1), jnp.float32),
            pltpu.SemaphoreType.DMA((8,)), pltpu.SemaphoreType.DMA((6, n_tp - 1)), pltpu.SemaphoreType.DMA((6, n_tp - 1)),
            pltpu.SemaphoreType.DMA((2, n_ep - 1)), pltpu.SemaphoreType.DMA((2, n_ep - 1)),
        ],
        compiler_params=pltpu.CompilerParams(vmem_limit_bytes=VMEM_LIMIT, collective_id=1, has_side_effects=True),
        name="block_b",
    )(h, ctx, scale, mask, idx_row, idx_col, router, w_out, w_cq, w_co, w_gate, w_up, w_down, cross_k, cross_v)


def decode_body(n_tp, n_ep, hidden, write_pos, enc_mask, expert_idx, self_keys, self_values, cross_keys, cross_values, rel_bias, norm_scale, w_query, w_key, w_value, w_out, w_cross_query, w_cross_out, dense_gate, dense_up, dense_down, router, exp_gate, exp_up, exp_down):
    lanes = lambda c: jnp.transpose(c, (0, 2, 3, 4, 1))
    sk, sv, ck, cv = lanes(self_keys), lanes(self_values), lanes(cross_keys), lanes(cross_values)
    flip = lambda w: jnp.swapaxes(w, 1, 2)
    wq, wk, wv, wcq = flip(w_query), flip(w_key), flip(w_value), flip(w_cross_query)
    pos = write_pos[None, :]
    mask = enc_mask.T
    caches = None
    h = hidden
    for layer in range(2):
        ctx, *caches = self_attention(layer, h, norm_scale[layer, 0:1], pos, rel_bias, wq[layer], wk[layer], wv[layer], sk, sv, caches)
        if layer == 0:
            h = dense_block(n_tp, layer, h, ctx, norm_scale[layer], mask, w_out, wcq, w_cross_out, dense_gate, dense_up, dense_down, ck, cv)
        else:
            h = moe_block(n_tp, n_ep, layer, h, ctx, norm_scale[layer], mask, expert_idx[None, :], expert_idx[:, None], router.T, w_out, wcq, w_cross_out, exp_gate, exp_up, exp_down, ck, cv)
    back = lambda c: jnp.transpose(c, (0, 4, 1, 2, 3))
    return h, back(caches[0]), back(caches[1])


def solution(mesh):
    batch = ('dp', 'ep')
    row_spec = P(batch, None)
    vec_spec = P(batch)
    cache_spec = P(None, batch, 'tp', None, None)
    col_spec = P(None, None, 'tp')
    out_rows = P(None, 'tp', None)
    in_specs = (row_spec, vec_spec, row_spec, vec_spec, cache_spec, cache_spec, cache_spec, cache_spec, P('tp', None), P(), col_spec, col_spec, col_spec, out_rows, col_spec, out_rows, P(None, 'tp'), P(None, 'tp'), P('tp', None), P(), P('ep', None, 'tp'), P('ep', None, 'tp'), P('ep', 'tp', None))
    out_specs = (row_spec, cache_spec, cache_spec)
    body = functools.partial(decode_body, mesh.shape['tp'], mesh.shape['ep'])
    return jax.shard_map(body, mesh=mesh, in_specs=in_specs, out_specs=out_specs, check_vma=False)
```

```python
import functools

import jax
import jax.numpy as jnp
from jax import lax
from jax.experimental import pallas as pl
from jax.experimental.pallas import tpu as pltpu
from jax.sharding import PartitionSpec as P

EPS = 1e-6
NEG_BIG = -1e9
MESH = pl.DeviceIdType.MESH
LANES = 128
VMEM = pl.BlockSpec(memory_space=pltpu.VMEM)
ANY = pl.BlockSpec(memory_space=pl.ANY)
VMEM_LIMIT = 48 * 1024 * 1024
OUT = pltpu.VMEM

NT = (((1,), (1,)), ((), ()))
NN = (((1,), (0,)), ((), ()))
TN = (((0,), (0,)), ((), ()))


def dot(a, b, dims=NN, **kw):
    return lax.dot_general(a, b, dims, preferred_element_type=jnp.float32, **kw)


def rms_norm(h, scale):
    h = h.astype(jnp.float32)
    inv = lax.rsqrt(jnp.mean(h * h, axis=-1, keepdims=True) + EPS)
    return (h * inv * scale).astype(jnp.bfloat16)


def softmax_rows(s):
    p = jnp.exp(s - jnp.max(s, axis=0, keepdims=True))
    return (p / jnp.sum(p, axis=0, keepdims=True)).astype(jnp.bfloat16).astype(jnp.float32)


def to_bf(mask):
    return mask.astype(jnp.float32).astype(jnp.bfloat16)


def enter(peers):
    barrier = pltpu.get_barrier_semaphore()
    for axis, index in peers:
        pl.semaphore_signal(barrier, inc=1, device_id={axis: index}, device_id_type=MESH)
    pl.semaphore_wait(barrier, len(peers))


def remote(src, dst, send_sem, recv_sem, device):
    copy = pltpu.make_async_remote_copy(src_ref=src, dst_ref=dst, send_sem=send_sem, recv_sem=recv_sem, device_id=device, device_id_type=MESH)
    copy.start()
    return copy


class Group:
    def __init__(self, axis, n, send, recv):
        self.axis, self.n, self.me = axis, n, lax.axis_index(axis)
        self.send, self.recv = send, recv

    def peer(self, k):
        return lax.rem(self.me + k, self.n)

    def peers(self):
        return [(self.axis, self.peer(k)) for k in range(1, self.n)]

    def copy_to(self, phase, k, src, dst):
        return remote(src, dst, self.send.at[phase, k - 1], self.recv.at[phase, k - 1], {self.axis: self.peer(k)})


class Spread:
    def __init__(self, slot, tp, ep, shard, full, send, recv):
        self.slot, self.tp, self.ep, self.shard, self.full, self.send, self.recv = slot, tp, ep, shard, full, send, recv
        rows, cols = shard.shape
        self.far = ep.n // 2
        self.half, self.place = lax.rem(ep.me, 2), ep.me // 2
        height, width = rows // self.far, cols // 2
        self.rows = pl.ds(pl.multiple_of(self.place * height, 16), height)
        self.cols = pl.ds(pl.multiple_of(self.half * width, LANES), width)
        self.copies, self.used = [], 0

    def _copy(self, src, dst, device):
        i = self.used
        self.used += 1
        copy = remote(src, dst, self.send.at[self.slot, i], self.recv.at[self.slot, i], device)
        self.copies.append(copy)
        return copy

    def over_tp(self):
        tp = self.tp
        self.first = [self._copy(self.shard.at[self.rows, self.cols], self.full.at[tp.me, self.rows, self.cols], {tp.axis: tp.peer(k)}) for k in range(1, tp.n)]

    def along_ep(self):
        for copy in self.first:
            copy.wait_recv()
        tp, ep = self.tp, self.ep
        self.second = []
        for m in range(1, self.far):
            there = lax.rem(self.place + m, self.far) * 2 + self.half
            for k in range(1, tp.n):
                piece = self.full.at[tp.peer(k), self.rows, self.cols]
                self.second.append(self._copy(piece, piece, {ep.axis: there}))

    def to_neighbour(self):
        for copy in self.second:
            copy.wait_recv()
        tp, ep = self.tp, self.ep
        there = self.place * 2 + 1 - self.half
        self.third = []
        for k in range(1, tp.n):
            piece = self.full.at[tp.peer(k), :, self.cols]
            self.third.append(self._copy(piece, piece, {ep.axis: there}))

    def finish(self):
        for copy in self.third:
            copy.wait_recv()


def routing(idx_row, experts):
    tokens = idx_row.shape[1]
    capacity = (2 * tokens + experts - 1) // experts
    one_t = lax.broadcasted_iota(jnp.int32, (experts, tokens), 0) == idx_row
    earlier = lax.broadcasted_iota(jnp.int32, (tokens, tokens), 0) < lax.broadcasted_iota(jnp.int32, (tokens, tokens), 1)
    count = dot(to_bf(one_t), to_bf(earlier))
    slot = jnp.sum(jnp.where(one_t, count, 0.0), axis=0, keepdims=True)
    place = jnp.where(slot < capacity, idx_row.astype(jnp.float32) * capacity + slot, -1.0)
    return place, one_t, capacity


def gelu_product(gate, up):
    return (jax.nn.gelu(gate) * up).astype(jnp.bfloat16)


def block_kernel(n_tp, n_ep, h_ref, scale_ref, pos_ref, mask_ref, bias_ref, idx_ref, router_ref,
                 wq_ref, wk_ref, wv_ref, wcq_ref, wo_ref, wco_ref, dg_ref, du_ref, dd_ref, eg_ref, eu_ref, ed_ref, sk_ref, sv_ref, ck_ref, cv_ref,
                 out_ref, ko_ref, vo_ref,
                 ck_buf, cv_buf, w_in, w_full, dg, du, dd, eg, eu, ed,
                 q_s, k_s, v_s, b_s, ctx_s, part_s, in_s, prod_s, h_s, disp, x_in, y_out, y_in, gate_s,
                 load_sem, cache_sem, tp_send, tp_recv, ctx_send, ctx_recv, ep_send, ep_recv, w_send, w_recv):
    heads, slots, dim, tokens = sk_ref.shape[1:]
    width = h_ref.shape[1]
    halves = tokens // LANES
    rows = tokens // n_tp
    tp = Group("tp", n_tp, tp_send, tp_recv)
    ep = Group("ep", n_ep, ep_send, ep_recv)
    sent = []

    pending = {}

    def load(name, src, dst):
        copy = pltpu.make_async_copy(src, dst, load_sem.at[len(pending)])
        copy.start()
        pending[name] = copy

    def ready(*names):
        for name in names:
            pending[name].wait()

    def cache_copies(which, layer, a):
        src = (sk_ref, sv_ref, ck_ref, cv_ref)[which].at[layer, a]
        dst = (ko_ref, vo_ref, ck_buf, cv_buf)[which].at[layer, a]
        return pltpu.make_async_copy(src, dst, cache_sem.at[which, layer, a])

    def load_caches(first, layer):
        for a in range(heads):
            cache_copies(first, layer, a).start()
            cache_copies(first + 1, layer, a).start()

    for i, ref in enumerate((wq_ref, wk_ref, wv_ref)):
        load(("w", 0, i), ref.at[0], w_in.at[0, i])
    load_caches(0, 0)
    enter(tp.peers() + ep.peers())

    spreads = [Spread(2 * layer + i, tp, ep, ref.at[layer], w_full.at[2 * layer + i], w_send, w_recv) for layer in range(2) for i, ref in enumerate((wo_ref, wco_ref))]
    spreads[0].over_tp()
    load(("full", 0), wo_ref.at[0], w_full.at[0, tp.me])
    load(("w", 0, 3), wcq_ref.at[0], w_in.at[0, 3])

    onehot = (lax.broadcasted_iota(jnp.int32, (LANES, tokens), 0) == pos_ref[...]).astype(jnp.float32)
    for a in range(heads):
        row = jnp.concatenate([bias_ref[a:a + 1, :], jnp.zeros((1, LANES - slots), jnp.float32)], axis=1)
        table = pltpu.roll(jnp.broadcast_to(row, (slots, LANES)), 0, 1, stride=1, stride_axis=0)
        b_s[a] = dot(table, onehot, precision=lax.Precision.HIGHEST)
    slot_id = lax.broadcasted_iota(jnp.int32, (slots, LANES), 0)

    def weighted(v_buf, a, cs, prob, acc):
        for j in range(slots):
            acc += v_buf[a, j, :, cs].astype(jnp.float32) * prob[j:j + 1, :]
        return acc

    def send_context(sub, a):
        mine = ctx_s.at[sub, tp.me, a]
        for k in range(1, n_tp):
            remote(mine, mine, ctx_send.at[sub, a, k - 1], ctx_recv.at[sub, a, k - 1], {"tp": tp.peer(k)})

    def context_copies(sub):
        mine = lambda a: ctx_s.at[sub, tp.me, a]
        return [pltpu.make_async_remote_copy(src_ref=mine(a), dst_ref=mine(a), send_sem=ctx_send.at[sub, a, k - 1], recv_sem=ctx_recv.at[sub, a, k - 1], device_id={"tp": tp.peer(k)}, device_id_type=MESH)
                for a in range(heads) for k in range(1, n_tp)]

    def out_project(sub, h, out):
        copies = context_copies(sub)
        for copy in copies:
            copy.wait_recv()
        spreads[sub].finish()
        ready(("full", sub))
        result = dot(ctx_s[sub].reshape(n_tp * heads * dim, tokens), w_full[sub].reshape(n_tp * heads * dim, width), TN)
        out[...] = (h[...].astype(jnp.float32) + result.astype(jnp.bfloat16).astype(jnp.float32)).astype(jnp.bfloat16)
        sent.extend(copies)

    def self_attention(layer, h, between=None):
        x = rms_norm(h[...], scale_ref[0, layer:layer + 1, :])
        ready(*[("w", layer, i) for i in range(3)])
        qt, kt, vt = (dot(w_in[layer, i], x, NT).astype(jnp.bfloat16) for i in range(3))
        for a in range(heads):
            q_s[a] = qt[a * dim:(a + 1) * dim, :].astype(jnp.float32)
            k_s[a] = kt[a * dim:(a + 1) * dim, :]
            v_s[a] = vt[a * dim:(a + 1) * dim, :]
        kb, vb = ko_ref.at[layer], vo_ref.at[layer]
        sub = 2 * layer

        def one_head(a, carry):
            cache_copies(0, layer, a).wait()
            cache_copies(1, layer, a).wait()
            for b in range(halves):
                cs = slice(b * LANES, (b + 1) * LANES)
                pos = pos_ref[:, cs]
                pos_bf = jnp.broadcast_to(pos.astype(jnp.float32), (dim, LANES)).astype(jnp.bfloat16)
                query, k_new, v_new = q_s[a, :, cs], k_s[a, :, cs], v_s[a, :, cs]
                parts = []
                for j in range(slots):
                    old = kb[a, j, :, cs]
                    kb[a, j, :, cs] = jnp.where(pos_bf == jnp.bfloat16(j), k_new, old)
                    parts.append(jnp.sum(old.astype(jnp.float32) * query, axis=0, keepdims=True))
                scores = jnp.concatenate(parts, axis=0)
                at_slot = slot_id == pos
                scores = jnp.where(at_slot, jnp.sum(k_new.astype(jnp.float32) * query, axis=0, keepdims=True), scores)
                prob = softmax_rows(jnp.where(slot_id <= pos, scores + b_s[a, :, cs], NEG_BIG))
                prob_new = jnp.sum(jnp.where(at_slot, prob, 0.0), axis=0, keepdims=True)
                prob_old = jnp.where(at_slot, 0.0, prob)
                acc = v_new.astype(jnp.float32) * prob_new
                for j in range(slots):
                    old = vb[a, j, :, cs]
                    vb[a, j, :, cs] = jnp.where(pos_bf == jnp.bfloat16(j), v_new, old)
                    acc += old.astype(jnp.float32) * prob_old[j:j + 1, :]
                ctx_s[sub, tp.me, a, :, cs] = acc.astype(jnp.bfloat16)
            send_context(sub, a)
            return carry

        lax.fori_loop(0, heads, one_head, 0)

    def cross_attention(layer, h):
        x = rms_norm(h[...], scale_ref[1, layer:layer + 1, :])
        ready(("w", layer, 3))
        qt = dot(w_in[layer, 3], x, NT).astype(jnp.bfloat16)
        for a in range(heads):
            q_s[a] = qt[a * dim:(a + 1) * dim, :].astype(jnp.float32)
        kb, vb = ck_buf.at[layer], cv_buf.at[layer]
        sub = 2 * layer + 1

        def one_head(a, carry):
            cache_copies(2, layer, a).wait()
            cache_copies(3, layer, a).wait()
            for b in range(halves):
                cs = slice(b * LANES, (b + 1) * LANES)
                query = q_s[a, :, cs]
                scores = jnp.concatenate([jnp.sum(kb[a, j, :, cs].astype(jnp.float32) * query, axis=0, keepdims=True) for j in range(slots)], axis=0)
                prob = softmax_rows(jnp.where(mask_ref[:, cs] > 0, scores, NEG_BIG))
                ctx_s[sub, tp.me, a, :, cs] = weighted(vb, a, cs, prob, jnp.zeros((dim, LANES), jnp.float32)).astype(jnp.bfloat16)
            send_context(sub, a)
            return carry

        lax.fori_loop(0, heads, one_head, 0)

    block = lambda i: pl.ds(pl.multiple_of(i * rows, rows), rows)

    def sum_over_tp(phase, part, h, out, gate=None):
        for k in (2, 1, 3)[:n_tp - 1] if n_tp == 4 else range(1, n_tp):
            part_s[phase, k] = part(tp.peer(k)).astype(jnp.bfloat16)
            sent.append(tp.copy_to(2 * phase, k, part_s.at[phase, k], in_s.at[phase, k - 1]))
        copies = sent[-(n_tp - 1):]
        total = part(tp.me)
        for copy in copies:
            copy.wait_recv()
        for k in range(n_tp - 1):
            total += in_s[phase, k].astype(jnp.float32)
        total = total.astype(jnp.bfloat16).astype(jnp.float32)
        if gate is not None:
            total = total * gate[block(tp.me), :]
        out[block(tp.me), :] = (h[block(tp.me), :].astype(jnp.float32) + total).astype(jnp.bfloat16)
        mine = out.at[block(tp.me)]
        copies = [tp.copy_to(2 * phase + 1, k, mine, mine) for k in range(1, n_tp)]
        for copy in copies:
            copy.wait_recv()
        sent.extend(copies)

    self_attention(0, h_ref)
    spreads[0].along_ep()
    spreads[1].over_tp()
    load(("full", 1), wco_ref.at[0], w_full.at[1, tp.me])
    load_caches(2, 0)
    for i, (name, ref, dst) in enumerate((("dg", dg_ref, dg), ("du", du_ref, du), ("dd", dd_ref, dd))):
        load(name, ref, dst)
    for i, ref in enumerate((wq_ref, wk_ref, wv_ref, wcq_ref)):
        load(("w", 1, i), ref.at[1], w_in.at[1, i])
    spreads[0].to_neighbour()
    spreads[1].along_ep()
    out_project(0, h_ref, h_s.at[0])
    for s in (2, 3):
        spreads[s].over_tp()
    load(("full", 2), wo_ref.at[1], w_full.at[2, tp.me])
    load(("full", 3), wco_ref.at[1], w_full.at[3, tp.me])
    load_caches(0, 1)
    cross_attention(0, h_s.at[0])
    spreads[1].to_neighbour()
    spreads[2].along_ep()
    out_project(1, h_s.at[0], h_s.at[1])
    load_caches(2, 1)
    for name, ref, dst in (("eg", eg_ref, eg), ("eu", eu_ref, eu), ("ed", ed_ref, ed)):
        load(name, ref, dst)
    x = rms_norm(h_s[1], scale_ref[2, 0:1, :])
    ready("dg", "du", "dd")
    prod_s[...] = gelu_product(dot(x, dg[...]), dot(x, du[...]))
    sum_over_tp(0, lambda i: dot(prod_s[block(i), :], dd[...]), h_s.at[1], h_s.at[2])
    spreads[2].to_neighbour()
    spreads[3].along_ep()

    self_attention(1, h_s.at[2])
    spreads[3].to_neighbour()
    out_project(2, h_s.at[2], h_s.at[3])
    cross_attention(1, h_s.at[3])
    experts = router_ref.shape[0]
    local = experts // n_ep
    place, one_t, capacity = routing(idx_ref[...], experts)
    spots = experts * capacity
    out_project(3, h_s.at[3], h_s.at[4])
    x = rms_norm(h_s[4], scale_ref[2, 1:2, :])
    pick = to_bf(lax.broadcasted_iota(jnp.int32, (spots, tokens), 0).astype(jnp.float32) == place)
    disp[...] = dot(pick, x).astype(jnp.bfloat16).reshape(disp.shape)
    there = [[ep.copy_to(j, k, disp.at[ep.peer(k), j], x_in.at[j, ep.me]) for k in range(1, n_ep)] for j in range(local)]
    logits = dot(router_ref[...], x.astype(jnp.float32), NT, precision=lax.Precision.HIGHEST)
    prob = jnp.exp(logits - jnp.max(logits, axis=0, keepdims=True))
    prob = prob / jnp.sum(prob, axis=0, keepdims=True)
    gate = jnp.sum(jnp.where(one_t, prob, 0.0), axis=0, keepdims=True)
    turned = jnp.concatenate([gate, place, jnp.zeros((LANES - 2, tokens), jnp.float32)], axis=0).T
    gate_s[...] = turned[:, 0:1]
    put = to_bf(lax.broadcasted_iota(jnp.int32, (tokens, spots), 1).astype(jnp.float32) == turned[:, 1:2])
    ready("eg", "eu", "ed")
    back = []
    for j in range(local):
        x_in[j, ep.me] = disp[ep.me, j]
        for copy in there[j]:
            copy.wait_recv()
        own = x_in[j].reshape(n_ep * capacity, width)
        product = gelu_product(dot(own, eg[j]), dot(own, eu[j]))
        y_out[:, j] = dot(product, ed[j]).astype(jnp.bfloat16).reshape(n_ep, capacity, width)
        y_in[ep.me, j] = y_out[ep.me, j]
        back += [ep.copy_to(local + j, k, y_out.at[ep.peer(k), j], y_in.at[ep.me, j]) for k in range(1, n_ep)]
    for copy in back:
        copy.wait_recv()
    prod_s[...] = dot(put, y_in[...].reshape(spots, width)).astype(jnp.bfloat16)
    sum_over_tp(1, lambda i: prod_s[block(i), :].astype(jnp.float32), h_s.at[4], out_ref, gate_s)
    for copy in sent + sum(there, []) + back:
        copy.wait_send()
    for spread in spreads:
        for copy in spread.copies:
            copy.wait_send()


def two_blocks(n_tp, n_ep, h, scale, pos, mask, bias, idx, router, weights, dense, expert, caches):
    tokens, width = h.shape
    sk, ck = caches[0], caches[2]
    _, heads, slots, dim, _ = sk.shape
    rows = tokens // n_tp
    experts = router.shape[0]
    local = experts // n_ep
    capacity = (2 * tokens + experts - 1) // experts
    bf = lambda *s: pltpu.VMEM(s, jnp.bfloat16)
    f32 = lambda *s: pltpu.VMEM(s, jnp.float32)
    dma = lambda *s: pltpu.SemaphoreType.DMA(s)
    shard = weights[-1].shape[1]
    pieces = 2 * (n_tp - 1) + (n_ep // 2 - 1) * (n_tp - 1)
    spots = (n_ep, local, capacity, width)
    return pl.pallas_call(
        functools.partial(block_kernel, n_tp, n_ep),
        out_shape=(OUT(h.shape, h.dtype), OUT(sk.shape, sk.dtype), OUT(sk.shape, sk.dtype)),
        in_specs=[VMEM] * 7 + [ANY] * 16,
        out_specs=(VMEM, VMEM, VMEM),
        scratch_shapes=[
            bf(*ck.shape), bf(*ck.shape), bf(2, 4, heads * dim, width), bf(4, n_tp, shard, width),
            *[bf(*w.shape) for w in dense], *[bf(*w.shape) for w in expert],
            f32(heads, dim, tokens), bf(heads, dim, tokens), bf(heads, dim, tokens), f32(heads, slots, tokens),
            bf(4, n_tp, heads, dim, tokens), bf(2, n_tp, rows, width), bf(2, n_tp - 1, rows, width), bf(tokens, width), bf(5, tokens, width),
            bf(*spots), bf(local, n_ep, capacity, width), bf(*spots), bf(*spots), f32(tokens, 1),
            dma(18), dma(4, 2, heads), dma(4, n_tp - 1), dma(4, n_tp - 1), dma(4, heads, n_tp - 1), dma(4, heads, n_tp - 1),
            dma(2 * local, n_ep - 1), dma(2 * local, n_ep - 1), dma(4, pieces), dma(4, pieces),
        ],
        compiler_params=pltpu.CompilerParams(vmem_limit_bytes=VMEM_LIMIT, collective_id=0, has_side_effects=True),
        name="two_blocks",
    )(h, scale, pos, mask, bias, idx, router, *weights, *dense, *expert, *caches)


def decode_body(n_tp, n_ep, hidden, write_pos, enc_mask, expert_idx, self_keys, self_values, cross_keys, cross_values, rel_bias, norm_scale, w_query, w_key, w_value, w_out, w_cross_query, w_cross_out, dense_gate, dense_up, dense_down, router, exp_gate, exp_up, exp_down):
    caches = [jnp.transpose(c, (0, 2, 3, 4, 1)) for c in (self_keys, self_values, cross_keys, cross_values)]
    flip = lambda w: jnp.swapaxes(w, 1, 2)
    weights = (flip(w_query), flip(w_key), flip(w_value), flip(w_cross_query), w_out, w_cross_out)
    h, keys, values = two_blocks(n_tp, n_ep, hidden, jnp.swapaxes(norm_scale, 0, 1), write_pos[None, :], enc_mask.T, rel_bias, expert_idx[None, :], router.T,
                                 weights, (dense_gate, dense_up, dense_down), (exp_gate, exp_up, exp_down), caches)
    back = lambda c: jnp.transpose(c, (0, 4, 1, 2, 3))
    return h, back(keys), back(values)


def solution(mesh):
    batch = ('dp', 'ep')
    row_spec = P(batch, None)
    vec_spec = P(batch)
    cache_spec = P(None, batch, 'tp', None, None)
    col_spec = P(None, None, 'tp')
    out_rows = P(None, 'tp', None)
    in_specs = (row_spec, vec_spec, row_spec, vec_spec, cache_spec, cache_spec, cache_spec, cache_spec, P('tp', None), P(), col_spec, col_spec, col_spec, out_rows, col_spec, out_rows, P(None, 'tp'), P(None, 'tp'), P('tp', None), P(), P('ep', None, 'tp'), P('ep', None, 'tp'), P('ep', 'tp', None))
    out_specs = (row_spec, cache_spec, cache_spec)
    body = functools.partial(decode_body, mesh.shape['tp'], mesh.shape['ep'])
    return jax.shard_map(body, mesh=mesh, in_specs=in_specs, out_specs=out_specs, check_vma=False)
```

```python
import functools

import jax
import jax.numpy as jnp
from jax import lax
from jax.experimental import pallas as pl
from jax.experimental.pallas import tpu as pltpu
from jax.sharding import PartitionSpec as P

EPS = 1e-6
NEG_BIG = -1e9
MESH = pl.DeviceIdType.MESH
LANES = 128
VMEM = pl.BlockSpec(memory_space=pltpu.VMEM)
ANY = pl.BlockSpec(memory_space=pl.ANY)
VMEM_LIMIT = 48 * 1024 * 1024
OUT = pltpu.VMEM
CHUNK = 256
DIRECT = 64

NT = (((1,), (1,)), ((), ()))
NN = (((1,), (0,)), ((), ()))
TN = (((0,), (0,)), ((), ()))


def dot(a, b, dims=NN, **kw):
    return lax.dot_general(a, b, dims, preferred_element_type=jnp.float32, **kw)


def rms_norm(h, scale):
    h = h.astype(jnp.float32)
    inv = lax.rsqrt(jnp.mean(h * h, axis=-1, keepdims=True) + EPS)
    return (h * inv * scale).astype(jnp.bfloat16)


def softmax_rows(s):
    p = jnp.exp(s - jnp.max(s, axis=0, keepdims=True))
    return (p / jnp.sum(p, axis=0, keepdims=True)).astype(jnp.bfloat16).astype(jnp.float32)


def to_bf(mask):
    return mask.astype(jnp.float32).astype(jnp.bfloat16)


def greet(peers):
    for axis, index in peers:
        pl.semaphore_signal(pltpu.get_barrier_semaphore(), inc=1, device_id={axis: index}, device_id_type=MESH)


def remote(src, dst, send_sem, recv_sem, device):
    copy = pltpu.make_async_remote_copy(src_ref=src, dst_ref=dst, send_sem=send_sem, recv_sem=recv_sem, device_id=device, device_id_type=MESH)
    copy.start()
    return copy


class Group:
    def __init__(self, axis, n, send, recv):
        self.axis, self.n, self.me = axis, n, lax.axis_index(axis)
        self.send, self.recv = send, recv

    def peer(self, k):
        return lax.rem(self.me + k, self.n)

    def peers(self):
        return [(self.axis, self.peer(k)) for k in range(1, self.n)]

    def copy_to(self, phase, k, src, dst):
        return remote(src, dst, self.send.at[phase, k - 1], self.recv.at[phase, k - 1], {self.axis: self.peer(k)})


class Spread:
    def __init__(self, slot, tp, ep, shard, full, send, recv, direct=0):
        self.slot, self.tp, self.ep, self.shard, self.full, self.send, self.recv = slot, tp, ep, shard, full, send, recv
        rows, cols = shard.shape
        self.far = ep.n // 2
        self.half, self.place = lax.rem(ep.me, 2), ep.me // 2
        self.direct, rows = direct, rows - direct
        height, width = rows // self.far, cols // 2
        self.rest = slice(rows, rows + direct)
        self.rows = pl.ds(pl.multiple_of(self.place * height, 16), height)
        self.cols = pl.ds(pl.multiple_of(self.half * width, LANES), width)
        self.copies, self.used = [], 0

    def _copy(self, src, dst, device):
        i = self.used
        self.used += 1
        copy = remote(src, dst, self.send.at[self.slot, i], self.recv.at[self.slot, i], device)
        self.copies.append(copy)
        return copy

    def over_tp(self):
        tp = self.tp
        self.first = [self._copy(self.shard.at[self.rows, self.cols], self.full.at[tp.me, self.rows, self.cols], {tp.axis: tp.peer(k)}) for k in range(1, tp.n)]
        self.extra = []
        if self.direct:
            self.extra = [self._copy(self.shard.at[self.rest, self.cols], self.full.at[tp.me, self.rest, self.cols], {tp.axis: tp.peer(k)}) for k in range(1, tp.n)]

    def along_ep(self):
        for copy in self.first:
            copy.wait_recv()
        tp, ep = self.tp, self.ep
        self.second = []
        for m in range(1, self.far):
            there = lax.rem(self.place + m, self.far) * 2 + self.half
            for k in range(1, tp.n):
                piece = self.full.at[tp.peer(k), self.rows, self.cols]
                self.second.append(self._copy(piece, piece, {ep.axis: there}))

    def to_neighbour(self):
        for copy in self.second + self.extra:
            copy.wait_recv()
        tp, ep = self.tp, self.ep
        there = self.place * 2 + 1 - self.half
        self.third = []
        for k in range(1, tp.n):
            piece = self.full.at[tp.peer(k), :, self.cols]
            self.third.append(self._copy(piece, piece, {ep.axis: there}))

    def finish(self):
        for copy in self.third:
            copy.wait_recv()


def routing(idx_row, experts):
    tokens = idx_row.shape[1]
    capacity = (2 * tokens + experts - 1) // experts
    one_t = lax.broadcasted_iota(jnp.int32, (experts, tokens), 0) == idx_row
    earlier = lax.broadcasted_iota(jnp.int32, (tokens, tokens), 0) < lax.broadcasted_iota(jnp.int32, (tokens, tokens), 1)
    count = dot(to_bf(one_t), to_bf(earlier))
    slot = jnp.sum(jnp.where(one_t, count, 0.0), axis=0, keepdims=True)
    place = jnp.where(slot < capacity, idx_row.astype(jnp.float32) * capacity + slot, -1.0)
    return place, one_t, capacity


def gelu_product(gate, up):
    return (jax.nn.gelu(gate) * up).astype(jnp.bfloat16)


def block_kernel(n_tp, n_ep, *refs):
    small, (h_ref, scale_ref, pos_ref, mask_ref, bias_ref, idx_ref, router_ref), refs = refs[:7], refs[-7:], refs[7:-7]
    (wq_ref, wk_ref, wv_ref, wcq_ref, wo_ref, wco_ref, dg_ref, du_ref, dd_ref, eg_ref, eu_ref, ed_ref, sk_ref, sv_ref, ck_ref, cv_ref,
                 out_ref, ko_ref, vo_ref,
                 ck_buf, cv_buf, w_in, w_full, dg, du, dd, eg, eu, ed,
                 q_s, k_s, v_s, b_s, ctx_s, part_s, in_s, prod_s, h_s, disp, x_in, y_out, y_in, gate_s,
                 load_sem, cache_sem, tp_send, tp_recv, ctx_send, ctx_recv, ep_send, ep_recv, w_send, w_recv) = refs
    heads, slots, dim, tokens = sk_ref.shape[1:]
    width = h_ref.shape[1]
    halves = tokens // LANES
    rows = tokens // n_tp
    tp = Group("tp", n_tp, tp_send, tp_recv)
    ep = Group("ep", n_ep, ep_send, ep_recv)
    greet(tp.peers() + ep.peers())
    sent = []

    pending = {}

    def load(name, src, dst):
        copy = pltpu.make_async_copy(src, dst, load_sem.at[len(pending)])
        copy.start()
        pending[name] = copy

    def ready(*names):
        for name in names:
            pending[name].wait()

    def cache_copies(which, layer, a):
        src = (sk_ref, sv_ref, ck_ref, cv_ref)[which].at[layer, a]
        dst = (ko_ref, vo_ref, ck_buf, cv_buf)[which].at[layer, a]
        return pltpu.make_async_copy(src, dst, cache_sem.at[which, layer, a])

    def load_caches(first, layer):
        for a in range(heads):
            cache_copies(first, layer, a).start()
            cache_copies(first + 1, layer, a).start()

    for i, (src, dst) in enumerate(zip(small, (h_ref, scale_ref, pos_ref, mask_ref, bias_ref, idx_ref, router_ref))):
        load(("small", i), src, dst)
    for i, ref in enumerate((wq_ref, wk_ref, wv_ref)):
        load(("w", 0, i), ref.at[0], w_in.at[0, i])
    load_caches(0, 0)
    pl.semaphore_wait(pltpu.get_barrier_semaphore(), n_tp + n_ep - 2)

    spreads = [Spread(2 * layer + i, tp, ep, ref.at[layer], w_full.at[2 * layer + i], w_send, w_recv, 0 if layer + i else DIRECT) for layer in range(2) for i, ref in enumerate((wo_ref, wco_ref))]
    spreads[0].over_tp()
    load(("full", 0), wo_ref.at[0], w_full.at[0, tp.me])
    load(("w", 0, 3), wcq_ref.at[0], w_in.at[0, 3])

    ready(*[("small", i) for i in range(7)])
    onehot = (lax.broadcasted_iota(jnp.int32, (LANES, tokens), 0) == pos_ref[...]).astype(jnp.float32)
    for a in range(heads):
        row = jnp.concatenate([bias_ref[a:a + 1, :], jnp.zeros((1, LANES - slots), jnp.float32)], axis=1)
        table = pltpu.roll(jnp.broadcast_to(row, (slots, LANES)), 0, 1, stride=1, stride_axis=0)
        b_s[a] = dot(table, onehot, precision=lax.Precision.HIGHEST)
    slot_id = lax.broadcasted_iota(jnp.int32, (slots, LANES), 0)

    def weighted(v_buf, a, cs, prob, acc):
        for j in range(slots):
            acc += v_buf[a, j, :, cs].astype(jnp.float32) * prob[j:j + 1, :]
        return acc

    def context_copy(sub, a, b, k):
        mine = ctx_s.at[sub, tp.me, a, :, pl.ds(b * LANES, LANES)]
        return pltpu.make_async_remote_copy(src_ref=mine, dst_ref=mine, send_sem=ctx_send.at[sub, a, b, k - 1], recv_sem=ctx_recv.at[sub, a, b, k - 1], device_id={"tp": tp.peer(k)}, device_id_type=MESH)

    def send_context(sub, a, b):
        for k in range(1, n_tp):
            context_copy(sub, a, b, k).start()

    def context_copies(sub):
        return [context_copy(sub, a, b, k) for a in range(heads) for b in range(halves) for k in range(1, n_tp)]

    def out_project(sub, h, out):
        copies = context_copies(sub)
        for copy in copies:
            copy.wait_recv()
        spreads[sub].finish()
        ready(("full", sub))
        result = dot(ctx_s[sub].reshape(n_tp * heads * dim, tokens), w_full[sub].reshape(n_tp * heads * dim, width), TN)
        out[...] = (h[...].astype(jnp.float32) + result.astype(jnp.bfloat16).astype(jnp.float32)).astype(jnp.bfloat16)
        sent.extend(copies)

    def self_attention(layer, h, between=None):
        x = rms_norm(h[...], scale_ref[0, layer:layer + 1, :])
        ready(*[("w", layer, i) for i in range(3)])
        qt, kt, vt = (dot(w_in[layer, i], x, NT).astype(jnp.bfloat16) for i in range(3))
        for a in range(heads):
            q_s[a] = qt[a * dim:(a + 1) * dim, :].astype(jnp.float32)
            k_s[a] = kt[a * dim:(a + 1) * dim, :]
            v_s[a] = vt[a * dim:(a + 1) * dim, :]
        kb, vb = ko_ref.at[layer], vo_ref.at[layer]
        sub = 2 * layer

        def one_head(a, carry):
            cache_copies(0, layer, a).wait()
            cache_copies(1, layer, a).wait()
            for b in range(halves):
                cs = slice(b * LANES, (b + 1) * LANES)
                pos = pos_ref[:, cs]
                pos_bf = jnp.broadcast_to(pos.astype(jnp.float32), (dim, LANES)).astype(jnp.bfloat16)
                query, k_new, v_new = q_s[a, :, cs], k_s[a, :, cs], v_s[a, :, cs]
                parts = []
                for j in range(slots):
                    old = kb[a, j, :, cs]
                    kb[a, j, :, cs] = jnp.where(pos_bf == jnp.bfloat16(j), k_new, old)
                    parts.append(jnp.sum(old.astype(jnp.float32) * query, axis=0, keepdims=True))
                scores = jnp.concatenate(parts, axis=0)
                at_slot = slot_id == pos
                scores = jnp.where(at_slot, jnp.sum(k_new.astype(jnp.float32) * query, axis=0, keepdims=True), scores)
                prob = softmax_rows(jnp.where(slot_id <= pos, scores + b_s[a, :, cs], NEG_BIG))
                prob_new = jnp.sum(jnp.where(at_slot, prob, 0.0), axis=0, keepdims=True)
                prob_old = jnp.where(at_slot, 0.0, prob)
                acc = v_new.astype(jnp.float32) * prob_new
                for j in range(slots):
                    old = vb[a, j, :, cs]
                    vb[a, j, :, cs] = jnp.where(pos_bf == jnp.bfloat16(j), v_new, old)
                    acc += old.astype(jnp.float32) * prob_old[j:j + 1, :]
                ctx_s[sub, tp.me, a, :, cs] = acc.astype(jnp.bfloat16)
                send_context(sub, a, b)
            return carry

        lax.fori_loop(0, heads, one_head, 0)

    def cross_attention(layer, h):
        x = rms_norm(h[...], scale_ref[1, layer:layer + 1, :])
        ready(("w", layer, 3))
        qt = dot(w_in[layer, 3], x, NT).astype(jnp.bfloat16)
        for a in range(heads):
            q_s[a] = qt[a * dim:(a + 1) * dim, :].astype(jnp.float32)
        kb, vb = ck_buf.at[layer], cv_buf.at[layer]
        sub = 2 * layer + 1

        def one_head(a, carry):
            cache_copies(2, layer, a).wait()
            cache_copies(3, layer, a).wait()
            for b in range(halves):
                cs = slice(b * LANES, (b + 1) * LANES)
                query = q_s[a, :, cs]
                scores = jnp.concatenate([jnp.sum(kb[a, j, :, cs].astype(jnp.float32) * query, axis=0, keepdims=True) for j in range(slots)], axis=0)
                prob = softmax_rows(jnp.where(mask_ref[:, cs] > 0, scores, NEG_BIG))
                ctx_s[sub, tp.me, a, :, cs] = weighted(vb, a, cs, prob, jnp.zeros((dim, LANES), jnp.float32)).astype(jnp.bfloat16)
                send_context(sub, a, b)
            return carry

        lax.fori_loop(0, heads, one_head, 0)

    block = lambda i: pl.ds(pl.multiple_of(i * rows, rows), rows)

    col = lambda c: slice(c * CHUNK, (c + 1) * CHUNK)
    chunks = width // CHUNK
    order = [n_tp // 2] + [k for k in range(1, n_tp) if k != n_tp // 2]

    def sum_over_tp(phase, prepare, part, h, out, gate=None, between=lambda: None):
        gathers, spreads_out = [], []
        for c in range(chunks):
            prepare(c)
            for k in order:
                part_s[phase, c, k] = part(tp.peer(k), c).astype(jnp.bfloat16)
                gathers.append(tp.copy_to((2 * phase) * chunks + c, k, part_s.at[phase, c, k], in_s.at[phase, c, k - 1]))
        own = [part(tp.me, c) for c in range(chunks)]
        between()
        for c in range(chunks):
            for copy in gathers[c * (n_tp - 1):(c + 1) * (n_tp - 1)]:
                copy.wait_recv()
            total = own[c]
            for k in range(n_tp - 1):
                total += in_s[phase, c, k].astype(jnp.float32)
            total = total.astype(jnp.bfloat16).astype(jnp.float32)
            if gate is not None:
                total = total * gate[block(tp.me), :]
            out[block(tp.me), col(c)] = (h[block(tp.me), col(c)].astype(jnp.float32) + total).astype(jnp.bfloat16)
            mine = out.at[block(tp.me), col(c)]
            spreads_out += [tp.copy_to((2 * phase + 1) * chunks + c, k, mine, mine) for k in order]
        for copy in spreads_out:
            copy.wait_recv()
        sent.extend(gathers + spreads_out)

    self_attention(0, h_ref)
    spreads[0].along_ep()
    for n in (1, 2, 3):
        spreads[n].over_tp()
    load(("full", 1), wco_ref.at[0], w_full.at[1, tp.me])
    load_caches(2, 0)
    for name, ref, dst in (("dg", dg_ref, dg), ("du", du_ref, du), ("dd", dd_ref, dd)):
        load(name, ref, dst)
    for i, ref in enumerate((wq_ref, wk_ref, wv_ref, wcq_ref)):
        load(("w", 1, i), ref.at[1], w_in.at[1, i])
    spreads[0].to_neighbour()
    spreads[1].along_ep()
    out_project(0, h_ref, h_s.at[0])
    load(("full", 2), wo_ref.at[1], w_full.at[2, tp.me])
    load(("full", 3), wco_ref.at[1], w_full.at[3, tp.me])
    load_caches(0, 1)
    cross_attention(0, h_s.at[0])
    spreads[1].to_neighbour()
    spreads[2].along_ep()
    out_project(1, h_s.at[0], h_s.at[1])
    load_caches(2, 1)
    for name, ref, dst in (("eg", eg_ref, eg), ("eu", eu_ref, eu), ("ed", ed_ref, ed)):
        load(name, ref, dst)
    x = rms_norm(h_s[1], scale_ref[2, 0:1, :])
    ready("dg", "du", "dd")
    prod_s[...] = gelu_product(dot(x, dg[...]), dot(x, du[...]))

    def move_weights():
        spreads[2].to_neighbour()
        spreads[3].along_ep()

    sum_over_tp(0, lambda c: None, lambda i, c: dot(prod_s[block(i), :], dd[:, col(c)]), h_s.at[1], h_s.at[2], between=move_weights)

    self_attention(1, h_s.at[2])
    spreads[3].to_neighbour()
    out_project(2, h_s.at[2], h_s.at[3])
    cross_attention(1, h_s.at[3])
    experts = router_ref.shape[0]
    local = experts // n_ep
    place, one_t, capacity = routing(idx_ref[...], experts)
    spots = experts * capacity
    out_project(3, h_s.at[3], h_s.at[4])
    x = rms_norm(h_s[4], scale_ref[2, 1:2, :])
    pick = to_bf(lax.broadcasted_iota(jnp.int32, (spots, tokens), 0).astype(jnp.float32) == place)
    disp[...] = dot(pick, x).astype(jnp.bfloat16).reshape(disp.shape)
    there = [[ep.copy_to(j, k, disp.at[ep.peer(k), j], x_in.at[j, ep.me]) for k in range(1, n_ep)] for j in range(local)]
    logits = dot(router_ref[...], x.astype(jnp.float32), NT, precision=lax.Precision.HIGHEST)
    prob = jnp.exp(logits - jnp.max(logits, axis=0, keepdims=True))
    prob = prob / jnp.sum(prob, axis=0, keepdims=True)
    gate = jnp.sum(jnp.where(one_t, prob, 0.0), axis=0, keepdims=True)
    turned = jnp.concatenate([gate, place, jnp.zeros((LANES - 2, tokens), jnp.float32)], axis=0).T
    gate_s[...] = turned[:, 0:1]
    put = to_bf(lax.broadcasted_iota(jnp.int32, (tokens, spots), 1).astype(jnp.float32) == turned[:, 1:2])
    ready("eg", "eu", "ed")
    back = {}
    for j in range(local):
        x_in[j, ep.me] = disp[ep.me, j]
        for copy in there[j]:
            copy.wait_recv()
        own = x_in[j].reshape(n_ep * capacity, width)
        product = gelu_product(dot(own, eg[j]), dot(own, eu[j]))
        for c in range(chunks):
            y_out[c, :, j] = dot(product, ed[j, :, col(c)]).astype(jnp.bfloat16).reshape(n_ep, capacity, CHUNK)
            y_in[c, ep.me, j] = y_out[c, ep.me, j]
            back[j, c] = [ep.copy_to(local + j * chunks + c, k, y_out.at[c, ep.peer(k), j], y_in.at[c, ep.me, j]) for k in range(1, n_ep)]

    def combine(c):
        for j in range(local):
            for copy in back[j, c]:
                copy.wait_recv()
        prod_s[:, col(c)] = dot(put, y_in[c].reshape(spots, CHUNK)).astype(jnp.bfloat16)

    sum_over_tp(1, combine, lambda i, c: prod_s[block(i), col(c)].astype(jnp.float32), h_s.at[4], out_ref, gate_s)
    back = sum(back.values(), [])
    for copy in sent + sum(there, []) + back:
        copy.wait_send()
    for spread in spreads:
        for copy in spread.copies:
            copy.wait_send()


def two_blocks(n_tp, n_ep, h, scale, pos, mask, bias, idx, router, weights, dense, expert, caches):
    tokens, width = h.shape
    sk, ck = caches[0], caches[2]
    _, heads, slots, dim, _ = sk.shape
    rows = tokens // n_tp
    experts = router.shape[0]
    local = experts // n_ep
    capacity = (2 * tokens + experts - 1) // experts
    bf = lambda *s: pltpu.VMEM(s, jnp.bfloat16)
    f32 = lambda *s: pltpu.VMEM(s, jnp.float32)
    dma = lambda *s: pltpu.SemaphoreType.DMA(s)
    shard = weights[-1].shape[1]
    pieces = 3 * (n_tp - 1) + (n_ep // 2 - 1) * (n_tp - 1)
    spots = (n_ep, local, capacity, width)
    chunks = width // CHUNK
    split = (chunks, n_ep, local, capacity, CHUNK)
    return pl.pallas_call(
        functools.partial(block_kernel, n_tp, n_ep),
        out_shape=(OUT(h.shape, h.dtype), OUT(sk.shape, sk.dtype), OUT(sk.shape, sk.dtype)),
        in_specs=[ANY] * 23,
        out_specs=(VMEM, VMEM, VMEM),
        scratch_shapes=[
            bf(*ck.shape), bf(*ck.shape), bf(2, 4, heads * dim, width), bf(4, n_tp, shard, width),
            *[bf(*w.shape) for w in dense], *[bf(*w.shape) for w in expert],
            f32(heads, dim, tokens), bf(heads, dim, tokens), bf(heads, dim, tokens), f32(heads, slots, tokens),
            bf(4, n_tp, heads, dim, tokens), bf(2, chunks, n_tp, rows, CHUNK), bf(2, chunks, n_tp - 1, rows, CHUNK), bf(tokens, width), bf(5, tokens, width),
            bf(*spots), bf(local, n_ep, capacity, width), bf(*split), bf(*split), f32(tokens, 1),
            dma(25), dma(4, 2, heads), dma(4 * chunks, n_tp - 1), dma(4 * chunks, n_tp - 1),
            dma(4, heads, tokens // LANES, n_tp - 1), dma(4, heads, tokens // LANES, n_tp - 1),
            dma(local * (1 + chunks), n_ep - 1), dma(local * (1 + chunks), n_ep - 1), dma(4, pieces), dma(4, pieces),
            *[pltpu.VMEM(a.shape, a.dtype) for a in (h, scale, pos, mask, bias, idx, router)],
        ],
        compiler_params=pltpu.CompilerParams(vmem_limit_bytes=VMEM_LIMIT, collective_id=0, has_side_effects=True),
        name="two_blocks",
    )(h, scale, pos, mask, bias, idx, router, *weights, *dense, *expert, *caches)


def decode_body(n_tp, n_ep, hidden, write_pos, enc_mask, expert_idx, self_keys, self_values, cross_keys, cross_values, rel_bias, norm_scale, w_query, w_key, w_value, w_out, w_cross_query, w_cross_out, dense_gate, dense_up, dense_down, router, exp_gate, exp_up, exp_down):
    caches = [jnp.transpose(c, (0, 2, 3, 4, 1)) for c in (self_keys, self_values, cross_keys, cross_values)]
    flip = lambda w: jnp.swapaxes(w, 1, 2)
    weights = (flip(w_query), flip(w_key), flip(w_value), flip(w_cross_query), w_out, w_cross_out)
    h, keys, values = two_blocks(n_tp, n_ep, hidden, jnp.swapaxes(norm_scale, 0, 1), write_pos[None, :], enc_mask.T, rel_bias, expert_idx[None, :], router.T,
                                 weights, (dense_gate, dense_up, dense_down), (exp_gate, exp_up, exp_down), caches)
    back = lambda c: jnp.transpose(c, (0, 4, 1, 2, 3))
    return h, back(keys), back(values)


def solution(mesh):
    batch = ('dp', 'ep')
    row_spec = P(batch, None)
    vec_spec = P(batch)
    cache_spec = P(None, batch, 'tp', None, None)
    col_spec = P(None, None, 'tp')
    out_rows = P(None, 'tp', None)
    in_specs = (row_spec, vec_spec, row_spec, vec_spec, cache_spec, cache_spec, cache_spec, cache_spec, P('tp', None), P(), col_spec, col_spec, col_spec, out_rows, col_spec, out_rows, P(None, 'tp'), P(None, 'tp'), P('tp', None), P(), P('ep', None, 'tp'), P('ep', None, 'tp'), P('ep', 'tp', None))
    out_specs = (row_spec, cache_spec, cache_spec)
    body = functools.partial(decode_body, mesh.shape['tp'], mesh.shape['ep'])
    return jax.shard_map(body, mesh=mesh, in_specs=in_specs, out_specs=out_specs, check_vma=False)
```

```python
import functools

import jax
import jax.numpy as jnp
from jax import lax
from jax.experimental import pallas as pl
from jax.experimental.pallas import tpu as pltpu
from jax.sharding import PartitionSpec as P

EPS = 1e-6
NEG_BIG = -1e9
MESH = pl.DeviceIdType.MESH
LANES = 128
VMEM = pl.BlockSpec(memory_space=pltpu.VMEM)
ANY = pl.BlockSpec(memory_space=pl.ANY)
VMEM_LIMIT = 48 * 1024 * 1024
OUT = pltpu.VMEM
CHUNK = 256
DIRECT = 64

NT = (((1,), (1,)), ((), ()))
NN = (((1,), (0,)), ((), ()))
TN = (((0,), (0,)), ((), ()))


def dot(a, b, dims=NN, **kw):
    return lax.dot_general(a, b, dims, preferred_element_type=jnp.float32, **kw)


def rms_norm(h, scale):
    h = h.astype(jnp.float32)
    inv = lax.rsqrt(jnp.mean(h * h, axis=-1, keepdims=True) + EPS)
    return (h * inv * scale).astype(jnp.bfloat16)


def softmax_rows(s):
    p = jnp.exp(s - jnp.max(s, axis=0, keepdims=True))
    return (p / jnp.sum(p, axis=0, keepdims=True)).astype(jnp.bfloat16).astype(jnp.float32)


def to_bf(mask):
    return mask.astype(jnp.float32).astype(jnp.bfloat16)


def greet(peers):
    for axis, index in peers:
        pl.semaphore_signal(pltpu.get_barrier_semaphore(), inc=1, device_id={axis: index}, device_id_type=MESH)


def remote(src, dst, send_sem, recv_sem, device):
    copy = pltpu.make_async_remote_copy(src_ref=src, dst_ref=dst, send_sem=send_sem, recv_sem=recv_sem, device_id=device, device_id_type=MESH)
    copy.start()
    return copy


class Group:
    def __init__(self, axis, n, send, recv):
        self.axis, self.n, self.me = axis, n, lax.axis_index(axis)
        self.send, self.recv = send, recv

    def peer(self, k):
        return lax.rem(self.me + k, self.n)

    def peers(self):
        return [(self.axis, self.peer(k)) for k in range(1, self.n)]

    def copy_to(self, phase, k, src, dst):
        return remote(src, dst, self.send.at[phase, k - 1], self.recv.at[phase, k - 1], {self.axis: self.peer(k)})


class Spread:
    def __init__(self, slot, tp, ep, shard, full, send, recv, direct=0):
        self.slot, self.tp, self.ep, self.shard, self.full, self.send, self.recv = slot, tp, ep, shard, full, send, recv
        rows, cols = shard.shape
        self.far = ep.n // 2
        self.half, self.place = lax.rem(ep.me, 2), ep.me // 2
        self.direct, rows = direct, rows - direct
        height, width = rows // self.far, cols // 2
        self.rest = slice(rows, rows + direct)
        self.rows = pl.ds(pl.multiple_of(self.place * height, 16), height)
        self.cols = pl.ds(pl.multiple_of(self.half * width, LANES), width)
        self.copies, self.used, self.extra = [], 0, []

    def _copy(self, src, dst, device):
        i = self.used
        self.used += 1
        copy = remote(src, dst, self.send.at[self.slot, i], self.recv.at[self.slot, i], device)
        self.copies.append(copy)
        return copy

    def over_tp(self):
        tp = self.tp
        self.first = [self._copy(self.shard.at[self.rows, self.cols], self.full.at[tp.me, self.rows, self.cols], {tp.axis: tp.peer(k)}) for k in range(1, tp.n)]

    def over_tp_direct(self):
        tp = self.tp
        if self.direct:
            self.extra = [self._copy(self.shard.at[self.rest, self.cols], self.full.at[tp.me, self.rest, self.cols], {tp.axis: tp.peer(k)}) for k in range(1, tp.n)]

    def along_ep(self):
        for copy in self.first:
            copy.wait_recv()
        tp, ep = self.tp, self.ep
        self.second = []
        for m in range(1, self.far):
            there = lax.rem(self.place + m, self.far) * 2 + self.half
            for k in range(1, tp.n):
                piece = self.full.at[tp.peer(k), self.rows, self.cols]
                self.second.append(self._copy(piece, piece, {ep.axis: there}))

    def to_neighbour(self):
        for copy in self.second + self.extra:
            copy.wait_recv()
        tp, ep = self.tp, self.ep
        there = self.place * 2 + 1 - self.half
        self.third = []
        for k in range(1, tp.n):
            piece = self.full.at[tp.peer(k), :, self.cols]
            self.third.append(self._copy(piece, piece, {ep.axis: there}))

    def finish(self):
        for copy in self.third:
            copy.wait_recv()


def routing(idx_row, experts):
    tokens = idx_row.shape[1]
    capacity = (2 * tokens + experts - 1) // experts
    one_t = lax.broadcasted_iota(jnp.int32, (experts, tokens), 0) == idx_row
    earlier = lax.broadcasted_iota(jnp.int32, (tokens, tokens), 0) < lax.broadcasted_iota(jnp.int32, (tokens, tokens), 1)
    count = dot(to_bf(one_t), to_bf(earlier))
    slot = jnp.sum(jnp.where(one_t, count, 0.0), axis=0, keepdims=True)
    place = jnp.where(slot < capacity, idx_row.astype(jnp.float32) * capacity + slot, -1.0)
    return place, one_t, capacity


def gelu_product(gate, up):
    return (jax.nn.gelu(gate) * up).astype(jnp.bfloat16)


def block_kernel(n_tp, n_ep, *refs):
    small, (h_ref, scale_ref, pos_ref, mask_ref, bias_ref, idx_ref, router_ref), refs = refs[:7], refs[-7:], refs[7:-7]
    (wq_ref, wk_ref, wv_ref, wcq_ref, wo_ref, wco_ref, dg_ref, du_ref, dd_ref, eg_ref, eu_ref, ed_ref, sk_ref, sv_ref, ck_ref, cv_ref,
                 out_ref, ko_ref, vo_ref,
                 ck_buf, cv_buf, w_in, w_full, dg, du, dd, eg, eu, ed,
                 q_s, k_s, v_s, b_s, ctx_s, part_s, in_s, part_d, in_d, prod_s, h_s, disp, x_in, y_out, y_in, gate_s,
                 load_sem, cache_sem, tp_send, tp_recv, ctx_send, ctx_recv, ep_send, ep_recv, w_send, w_recv) = refs
    heads, slots, dim, tokens = sk_ref.shape[1:]
    width = h_ref.shape[1]
    halves = tokens // LANES
    rows = tokens // n_tp
    tp = Group("tp", n_tp, tp_send, tp_recv)
    ep = Group("ep", n_ep, ep_send, ep_recv)
    greet(tp.peers() + ep.peers())
    sent = []

    pending = {}

    def load(name, src, dst):
        copy = pltpu.make_async_copy(src, dst, load_sem.at[len(pending)])
        copy.start()
        pending[name] = copy

    def ready(*names):
        for name in names:
            pending[name].wait()

    def cache_copies(which, layer, a):
        src = (sk_ref, sv_ref, ck_ref, cv_ref)[which].at[layer, a]
        dst = (ko_ref, vo_ref, ck_buf, cv_buf)[which].at[layer, a]
        return pltpu.make_async_copy(src, dst, cache_sem.at[which, layer, a])

    def load_caches(first, layer):
        for a in range(heads):
            cache_copies(first, layer, a).start()
            cache_copies(first + 1, layer, a).start()

    for i, (src, dst) in enumerate(zip(small, (h_ref, scale_ref, pos_ref, mask_ref, bias_ref, idx_ref, router_ref))):
        load(("small", i), src, dst)
    for i, ref in enumerate((wq_ref, wk_ref, wv_ref)):
        load(("w", 0, i), ref.at[0], w_in.at[0, i])
    load_caches(0, 0)
    pl.semaphore_wait(pltpu.get_barrier_semaphore(), n_tp + n_ep - 2)

    spreads = [Spread(2 * layer + i, tp, ep, ref.at[layer], w_full.at[2 * layer + i], w_send, w_recv, 0 if layer else DIRECT) for layer in range(2) for i, ref in enumerate((wo_ref, wco_ref))]
    spreads[0].over_tp()
    spreads[0].over_tp_direct()
    load(("full", 0), wo_ref.at[0], w_full.at[0, tp.me])
    load(("w", 0, 3), wcq_ref.at[0], w_in.at[0, 3])

    ready(*[("small", i) for i in range(7)])
    onehot = (lax.broadcasted_iota(jnp.int32, (LANES, tokens), 0) == pos_ref[...]).astype(jnp.float32)
    for a in range(heads):
        row = jnp.concatenate([bias_ref[a:a + 1, :], jnp.zeros((1, LANES - slots), jnp.float32)], axis=1)
        table = pltpu.roll(jnp.broadcast_to(row, (slots, LANES)), 0, 1, stride=1, stride_axis=0)
        b_s[a] = dot(table, onehot, precision=lax.Precision.HIGHEST)
    slot_id = lax.broadcasted_iota(jnp.int32, (slots, LANES), 0)

    def context_copy(sub, a, b, k):
        mine = ctx_s.at[sub, tp.me, a, :, pl.ds(b * LANES, LANES)]
        return pltpu.make_async_remote_copy(src_ref=mine, dst_ref=mine, send_sem=ctx_send.at[sub, a, b, k - 1], recv_sem=ctx_recv.at[sub, a, b, k - 1], device_id={"tp": tp.peer(k)}, device_id_type=MESH)

    def send_context(sub, a, b):
        for k in range(1, n_tp):
            context_copy(sub, a, b, k).start()

    def lanes(b):
        return slice(b * LANES, (b + 1) * LANES)

    def out_project(sub, h, out, b):
        copies = [context_copy(sub, a, b, k) for a in range(heads) for k in range(1, n_tp)]
        for copy in copies:
            copy.wait_recv()
        if b == 0:
            spreads[sub].finish()
            ready(("full", sub))
        result = dot(ctx_s[sub, :, :, :, lanes(b)].reshape(n_tp * heads * dim, LANES), w_full[sub].reshape(n_tp * heads * dim, width), TN)
        out[lanes(b), :] = (h[lanes(b), :].astype(jnp.float32) + result.astype(jnp.bfloat16).astype(jnp.float32)).astype(jnp.bfloat16)
        sent.extend(copies)

    def self_attention(layer, h, b):
        cs = lanes(b)
        x = rms_norm(h[cs, :], scale_ref[0, layer:layer + 1, :])
        if b == 0:
            ready(*[("w", layer, i) for i in range(3)])
        qt, kt, vt = (dot(w_in[layer, i], x, NT).astype(jnp.bfloat16) for i in range(3))
        for a in range(heads):
            q_s[a, :, cs] = qt[a * dim:(a + 1) * dim, :].astype(jnp.float32)
            k_s[a, :, cs] = kt[a * dim:(a + 1) * dim, :]
            v_s[a, :, cs] = vt[a * dim:(a + 1) * dim, :]
        kb, vb = ko_ref.at[layer], vo_ref.at[layer]
        sub = 2 * layer
        pos = pos_ref[:, cs]
        pos_bf = jnp.broadcast_to(pos.astype(jnp.float32), (dim, LANES)).astype(jnp.bfloat16)

        def one_head(a, carry):
            if b == 0:
                cache_copies(0, layer, a).wait()
                cache_copies(1, layer, a).wait()
            query, k_new, v_new = q_s[a, :, cs], k_s[a, :, cs], v_s[a, :, cs]
            parts = []
            for j in range(slots):
                old = kb[a, j, :, cs]
                kb[a, j, :, cs] = jnp.where(pos_bf == jnp.bfloat16(j), k_new, old)
                parts.append(jnp.sum(old.astype(jnp.float32) * query, axis=0, keepdims=True))
            scores = jnp.concatenate(parts, axis=0)
            at_slot = slot_id == pos
            scores = jnp.where(at_slot, jnp.sum(k_new.astype(jnp.float32) * query, axis=0, keepdims=True), scores)
            prob = softmax_rows(jnp.where(slot_id <= pos, scores + b_s[a, :, cs], NEG_BIG))
            prob_new = jnp.sum(jnp.where(at_slot, prob, 0.0), axis=0, keepdims=True)
            prob_old = jnp.where(at_slot, 0.0, prob)
            acc = v_new.astype(jnp.float32) * prob_new
            for j in range(slots):
                old = vb[a, j, :, cs]
                vb[a, j, :, cs] = jnp.where(pos_bf == jnp.bfloat16(j), v_new, old)
                acc += old.astype(jnp.float32) * prob_old[j:j + 1, :]
            ctx_s[sub, tp.me, a, :, cs] = acc.astype(jnp.bfloat16)
            send_context(sub, a, b)
            return carry

        lax.fori_loop(0, heads, one_head, 0)

    def cross_attention(layer, h, b):
        cs = lanes(b)
        x = rms_norm(h[cs, :], scale_ref[1, layer:layer + 1, :])
        if b == 0:
            ready(("w", layer, 3))
        qt = dot(w_in[layer, 3], x, NT).astype(jnp.bfloat16)
        for a in range(heads):
            q_s[a, :, cs] = qt[a * dim:(a + 1) * dim, :].astype(jnp.float32)
        kb, vb = ck_buf.at[layer], cv_buf.at[layer]
        sub = 2 * layer + 1

        def one_head(a, carry):
            if b == 0:
                cache_copies(2, layer, a).wait()
                cache_copies(3, layer, a).wait()
            query = q_s[a, :, cs]
            scores = jnp.concatenate([jnp.sum(kb[a, j, :, cs].astype(jnp.float32) * query, axis=0, keepdims=True) for j in range(slots)], axis=0)
            prob = softmax_rows(jnp.where(mask_ref[:, cs] > 0, scores, NEG_BIG))
            acc = jnp.zeros((dim, LANES), jnp.float32)
            for j in range(slots):
                acc += vb[a, j, :, cs].astype(jnp.float32) * prob[j:j + 1, :]
            ctx_s[sub, tp.me, a, :, cs] = acc.astype(jnp.bfloat16)
            send_context(sub, a, b)
            return carry

        lax.fori_loop(0, heads, one_head, 0)

    block = lambda i: pl.ds(pl.multiple_of(i * rows, rows), rows)

    col = lambda c: slice(c * CHUNK, (c + 1) * CHUNK)
    chunks = width // CHUNK
    order = [n_tp // 2] + [k for k in range(1, n_tp) if k != n_tp // 2]

    def sum_over_tp(prepare, part, h, out, gate):
        gathers, spreads_out = [], []
        for c in range(chunks):
            prepare(c)
            for k in order:
                part_s[c, k] = part(tp.peer(k), c).astype(jnp.bfloat16)
                gathers.append(tp.copy_to(2 * halves + c, k, part_s.at[c, k], in_s.at[c, k - 1]))
        own = [part(tp.me, c) for c in range(chunks)]
        for c in range(chunks):
            for copy in gathers[c * (n_tp - 1):(c + 1) * (n_tp - 1)]:
                copy.wait_recv()
            total = own[c]
            for k in range(n_tp - 1):
                total += in_s[c, k].astype(jnp.float32)
            total = total.astype(jnp.bfloat16).astype(jnp.float32)
            total = total * gate[block(tp.me), :]
            out[block(tp.me), col(c)] = (h[block(tp.me), col(c)].astype(jnp.float32) + total).astype(jnp.bfloat16)
            mine = out.at[block(tp.me), col(c)]
            spreads_out += [tp.copy_to(2 * halves + chunks + c, k, mine, mine) for k in order]
        for copy in spreads_out:
            copy.wait_recv()
        sent.extend(gathers + spreads_out)

    own_rows = rows // halves
    half_block = lambda b, i: pl.ds(pl.multiple_of(b * LANES + i * own_rows, own_rows), own_rows)
    half_in, half_out = {}, {}

    def half_parts(b, part):
        part_d[b] = part.astype(jnp.bfloat16)
        there = lambda k: part_d.at[b, pl.ds(pl.multiple_of(tp.peer(k) * own_rows, own_rows), own_rows)]
        half_in[b] = [tp.copy_to(b, k, there(k), in_d.at[b, k - 1]) for k in order]

    def half_sums(b, h, out):
        for copy in half_in[b]:
            copy.wait_recv()
        total = part_d[b, pl.ds(pl.multiple_of(tp.me * own_rows, own_rows), own_rows), :].astype(jnp.float32)
        for k in range(n_tp - 1):
            total += in_d[b, k].astype(jnp.float32)
        mine = half_block(b, tp.me)
        out[mine, :] = (h[mine, :].astype(jnp.float32) + total.astype(jnp.bfloat16).astype(jnp.float32)).astype(jnp.bfloat16)
        half_out[b] = [tp.copy_to(halves + b, k, out.at[mine], out.at[mine]) for k in order]

    def half_arrived(b):
        for copy in half_out[b]:
            copy.wait_recv()
        sent.extend(half_in[b] + half_out[b])

    self_attention(0, h_ref, 0)
    spreads[1].over_tp()
    for b in range(1, halves):
        self_attention(0, h_ref, b)
    spreads[0].along_ep()
    spreads[2].over_tp()
    spreads[1].over_tp_direct()
    load(("full", 1), wco_ref.at[0], w_full.at[1, tp.me])
    load_caches(2, 0)
    for name, ref, dst in (("dg", dg_ref, dg), ("du", du_ref, du), ("dd", dd_ref, dd)):
        load(name, ref, dst)
    for i, ref in enumerate((wq_ref, wk_ref, wv_ref, wcq_ref)):
        load(("w", 1, i), ref.at[1], w_in.at[1, i])
    spreads[0].to_neighbour()
    spreads[1].along_ep()
    for b in range(halves):
        out_project(0, h_ref, h_s.at[0], b)
        cross_attention(0, h_s.at[0], b)
    load(("full", 2), wo_ref.at[1], w_full.at[2, tp.me])
    load(("full", 3), wco_ref.at[1], w_full.at[3, tp.me])
    load_caches(0, 1)
    spreads[1].to_neighbour()
    spreads[2].along_ep()
    load_caches(2, 1)
    for name, ref, dst in (("eg", eg_ref, eg), ("eu", eu_ref, eu), ("ed", ed_ref, ed)):
        load(name, ref, dst)
    for b in range(halves):
        out_project(1, h_s.at[0], h_s.at[1], b)
        x = rms_norm(h_s[1, lanes(b), :], scale_ref[2, 0:1, :])
        if b == 0:
            ready("dg", "du", "dd")
        half_parts(b, dot(gelu_product(dot(x, dg[...]), dot(x, du[...])), dd[...]))
        if b == 0:
            spreads[3].over_tp()
    for b in range(halves):
        half_sums(b, h_s.at[1], h_s.at[2])
        if b == 0:
            spreads[3].along_ep()
            spreads[2].to_neighbour()
    for b in range(halves):
        half_arrived(b)
        self_attention(1, h_s.at[2], b)
    spreads[3].to_neighbour()
    for b in range(halves):
        out_project(2, h_s.at[2], h_s.at[3], b)
        cross_attention(1, h_s.at[3], b)
    experts = router_ref.shape[0]
    local = experts // n_ep
    place, one_t, capacity = routing(idx_ref[...], experts)
    spots = experts * capacity
    for b in range(halves):
        out_project(3, h_s.at[3], h_s.at[4], b)
    x = rms_norm(h_s[4], scale_ref[2, 1:2, :])
    pick = to_bf(lax.broadcasted_iota(jnp.int32, (spots, tokens), 0).astype(jnp.float32) == place)
    disp[...] = dot(pick, x).astype(jnp.bfloat16).reshape(disp.shape)
    there = [[ep.copy_to(j, k, disp.at[ep.peer(k), j], x_in.at[j, ep.me]) for k in range(1, n_ep)] for j in range(local)]
    logits = dot(router_ref[...], x.astype(jnp.float32), NT, precision=lax.Precision.HIGHEST)
    prob = jnp.exp(logits - jnp.max(logits, axis=0, keepdims=True))
    prob = prob / jnp.sum(prob, axis=0, keepdims=True)
    gate = jnp.sum(jnp.where(one_t, prob, 0.0), axis=0, keepdims=True)
    turned = jnp.concatenate([gate, place, jnp.zeros((LANES - 2, tokens), jnp.float32)], axis=0).T
    gate_s[...] = turned[:, 0:1]
    put = to_bf(lax.broadcasted_iota(jnp.int32, (tokens, spots), 1).astype(jnp.float32) == turned[:, 1:2])
    ready("eg", "eu", "ed")
    back = {}
    for j in range(local):
        x_in[j, ep.me] = disp[ep.me, j]
        for copy in there[j]:
            copy.wait_recv()
        own = x_in[j].reshape(n_ep * capacity, width)
        product = gelu_product(dot(own, eg[j]), dot(own, eu[j]))
        for c in range(chunks):
            y_out[c, :, j] = dot(product, ed[j, :, col(c)]).astype(jnp.bfloat16).reshape(n_ep, capacity, CHUNK)
            y_in[c, ep.me, j] = y_out[c, ep.me, j]
            back[j, c] = [ep.copy_to(local + j * chunks + c, k, y_out.at[c, ep.peer(k), j], y_in.at[c, ep.me, j]) for k in range(1, n_ep)]

    def combine(c):
        for j in range(local):
            for copy in back[j, c]:
                copy.wait_recv()
        prod_s[:, col(c)] = dot(put, y_in[c].reshape(spots, CHUNK)).astype(jnp.bfloat16)

    sum_over_tp(combine, lambda i, c: prod_s[block(i), col(c)].astype(jnp.float32), h_s.at[4], out_ref, gate_s)
    back = sum(back.values(), [])
    for copy in sent + sum(there, []) + back:
        copy.wait_send()
    for spread in spreads:
        for copy in spread.copies:
            copy.wait_send()


def two_blocks(n_tp, n_ep, h, scale, pos, mask, bias, idx, router, weights, dense, expert, caches):
    tokens, width = h.shape
    sk, ck = caches[0], caches[2]
    _, heads, slots, dim, _ = sk.shape
    rows = tokens // n_tp
    experts = router.shape[0]
    local = experts // n_ep
    capacity = (2 * tokens + experts - 1) // experts
    bf = lambda *s: pltpu.VMEM(s, jnp.bfloat16)
    f32 = lambda *s: pltpu.VMEM(s, jnp.float32)
    dma = lambda *s: pltpu.SemaphoreType.DMA(s)
    shard = weights[-1].shape[1]
    pieces = 3 * (n_tp - 1) + (n_ep // 2 - 1) * (n_tp - 1)
    spots = (n_ep, local, capacity, width)
    chunks, halves = width // CHUNK, tokens // LANES
    split = (chunks, n_ep, local, capacity, CHUNK)
    return pl.pallas_call(
        functools.partial(block_kernel, n_tp, n_ep),
        out_shape=(OUT(h.shape, h.dtype), OUT(sk.shape, sk.dtype), OUT(sk.shape, sk.dtype)),
        in_specs=[ANY] * 23,
        out_specs=(VMEM, VMEM, VMEM),
        scratch_shapes=[
            bf(*ck.shape), bf(*ck.shape), bf(2, 4, heads * dim, width), bf(4, n_tp, shard, width),
            *[bf(*w.shape) for w in dense], *[bf(*w.shape) for w in expert],
            f32(heads, dim, tokens), bf(heads, dim, tokens), bf(heads, dim, tokens), f32(heads, slots, tokens),
            bf(4, n_tp, heads, dim, tokens), bf(chunks, n_tp, rows, CHUNK), bf(chunks, n_tp - 1, rows, CHUNK), bf(halves, LANES, width), bf(halves, n_tp - 1, LANES // n_tp, width), bf(tokens, width), bf(5, tokens, width),
            bf(*spots), bf(local, n_ep, capacity, width), bf(*split), bf(*split), f32(tokens, 1),
            dma(25), dma(4, 2, heads), dma(2 * (halves + chunks), n_tp - 1), dma(2 * (halves + chunks), n_tp - 1),
            dma(4, heads, tokens // LANES, n_tp - 1), dma(4, heads, tokens // LANES, n_tp - 1),
            dma(local * (1 + chunks), n_ep - 1), dma(local * (1 + chunks), n_ep - 1), dma(4, pieces), dma(4, pieces),
            *[pltpu.VMEM(a.shape, a.dtype) for a in (h, scale, pos, mask, bias, idx, router)],
        ],
        compiler_params=pltpu.CompilerParams(vmem_limit_bytes=VMEM_LIMIT, collective_id=0, has_side_effects=True),
        name="two_blocks",
    )(h, scale, pos, mask, bias, idx, router, *weights, *dense, *expert, *caches)


def decode_body(n_tp, n_ep, hidden, write_pos, enc_mask, expert_idx, self_keys, self_values, cross_keys, cross_values, rel_bias, norm_scale, w_query, w_key, w_value, w_out, w_cross_query, w_cross_out, dense_gate, dense_up, dense_down, router, exp_gate, exp_up, exp_down):
    caches = [jnp.transpose(c, (0, 2, 3, 4, 1)) for c in (self_keys, self_values, cross_keys, cross_values)]
    flip = lambda w: jnp.swapaxes(w, 1, 2)
    weights = (flip(w_query), flip(w_key), flip(w_value), flip(w_cross_query), w_out, w_cross_out)
    h, keys, values = two_blocks(n_tp, n_ep, hidden, jnp.swapaxes(norm_scale, 0, 1), write_pos[None, :], enc_mask.T, rel_bias, expert_idx[None, :], router.T,
                                 weights, (dense_gate, dense_up, dense_down), (exp_gate, exp_up, exp_down), caches)
    back = lambda c: jnp.transpose(c, (0, 4, 1, 2, 3))
    return h, back(keys), back(values)


def solution(mesh):
    batch = ('dp', 'ep')
    row_spec = P(batch, None)
    vec_spec = P(batch)
    cache_spec = P(None, batch, 'tp', None, None)
    col_spec = P(None, None, 'tp')
    out_rows = P(None, 'tp', None)
    in_specs = (row_spec, vec_spec, row_spec, vec_spec, cache_spec, cache_spec, cache_spec, cache_spec, P('tp', None), P(), col_spec, col_spec, col_spec, out_rows, col_spec, out_rows, P(None, 'tp'), P(None, 'tp'), P('tp', None), P(), P('ep', None, 'tp'), P('ep', None, 'tp'), P('ep', 'tp', None))
    out_specs = (row_spec, cache_spec, cache_spec)
    body = functools.partial(decode_body, mesh.shape['tp'], mesh.shape['ep'])
    return jax.shard_map(body, mesh=mesh, in_specs=in_specs, out_specs=out_specs, check_vma=False)
```
